8 devices in a mesh: dp: 2 (over z, y), tp: 4 (over x, core).
Axes of the slice: x: 2, y: 2, z: 1, core: 2. Of those that a mesh axis runs over, the one named last changes fastest.
Arguments:
- x: bfloat16 [16, 384, 7168], P('dp'), parts along dimension 0
- seq_lens: int32 [16], P('dp'), parts along dimension 0
- w_query: bfloat16 [7168, 7168], P(None, 'tp')
- w_key: bfloat16 [7168, 1024], P(None, 'tp')
- w_value: bfloat16 [7168, 1024], P(None, 'tp')
- w_out: bfloat16 [7168, 7168], P('tp')
- w_gate: bfloat16 [7168, 20480], P(None, 'tp')
- w_up: bfloat16 [7168, 20480], P(None, 'tp')
- w_down: bfloat16 [20480, 7168], P('tp')
- attn_gain: bfloat16 [7168], replicated
- mlp_gain: bfloat16 [7168], replicated
- k_cache: bfloat16 [16, 768, 8, 128], P('dp', None, 'tp'), parts along dimension 0
- v_cache: bfloat16 [16, 768, 8, 128], P('dp', None, 'tp'), parts along dimension 0
Outputs:
- output 1: bfloat16 [16, 384, 7168], P('dp'), parts along dimension 0
- output 2: bfloat16 [16, 768, 8, 128], P('dp', None, 'tp'), parts along dimension 0
- output 3: bfloat16 [16, 768, 8, 128], P('dp', None, 'tp'), parts along dimension 0
There are 2 independent parts. The reference program is written for one: setup_inputs(seed, part) draws one part's arguments, and reference() takes and returns one part's arrays. A program takes and returns all parts, laid end to end along the dimension named above; an argument that names none is the same for every part.
All inputs are finite; a program needn't handle non-finite values.
Results may differ from the reference program's by a relative error of at most 0.0113591.
Values are sent between devices in bfloat16 or wider.
A program may use at most 1.5 GiB of HBM per device.

```python
import jax
import jax.numpy as jnp
from jax import lax

D = 7168
HEADS = 56
KV_HEADS = 8
HEAD = 128
FF = 20480
BATCH = 8
SEQ = 384
CACHE_LEN = 768
TP = 4
EPS = 1e-5
ROPE_BASE = 10000.0


def setup_inputs(seed: int = 0, part: int = 0) -> dict:
    base_key = jax.random.key(seed)
    part_key = jax.random.fold_in(base_key, part)
    weight_keys = jax.random.split(base_key, 9)
    part_keys = jax.random.split(part_key, 5)
    qk_scale = 1.5 * D ** -0.5

    def normal_weight(rng_key, array_shape, factor):
        return (jax.random.normal(rng_key, array_shape, jnp.float32) * factor).astype(jnp.bfloat16)

    short_len = jax.random.randint(part_keys[1], (1,), SEQ // 2, (4 * SEQ) // 5 + 1)
    other_lens = jax.random.randint(part_keys[2], (BATCH - 1,), SEQ // 2, SEQ + 1)
    return {
        "x": normal_weight(part_keys[0], (BATCH, SEQ, D), 1.0),
        "seq_lens": jnp.concatenate([short_len, other_lens]).astype(jnp.int32),
        "w_query": normal_weight(weight_keys[0], (D, HEADS * HEAD), qk_scale),
        "w_key": normal_weight(weight_keys[1], (D, KV_HEADS * HEAD), qk_scale),
        "w_value": normal_weight(weight_keys[2], (D, KV_HEADS * HEAD), D ** -0.5),
        "w_out": normal_weight(weight_keys[3], (HEADS * HEAD, D), (HEADS * HEAD) ** -0.5),
        "w_gate": normal_weight(weight_keys[4], (D, FF), D ** -0.5),
        "w_up": normal_weight(weight_keys[5], (D, FF), D ** -0.5),
        "w_down": normal_weight(weight_keys[6], (FF, D), FF ** -0.5),
        "attn_gain": jax.random.uniform(weight_keys[7], (D,), jnp.float32, 0.5, 1.5).astype(jnp.bfloat16),
        "mlp_gain": jax.random.uniform(weight_keys[8], (D,), jnp.float32, 0.5, 1.5).astype(jnp.bfloat16),
        "k_cache": normal_weight(part_keys[3], (BATCH, CACHE_LEN, KV_HEADS, HEAD), 1.0),
        "v_cache": normal_weight(part_keys[4], (BATCH, CACHE_LEN, KV_HEADS, HEAD), 1.0),
    }


def rms_norm(rows, gain):
    rows32 = rows.astype(jnp.float32)
    inv_rms = lax.rsqrt(jnp.mean(rows32 * rows32, axis=-1, keepdims=True) + EPS)
    return (rows32 * inv_rms * gain.astype(jnp.float32)).astype(jnp.bfloat16)


def rotary(vecs, angles):
    half_dim = HEAD // 2
    pairs = vecs.reshape(vecs.shape[:-1] + (half_dim, 2))
    even_part = pairs[..., 0]
    odd_part = pairs[..., 1]
    cos_tab = jnp.cos(angles)[:, None, :]
    sin_tab = jnp.sin(angles)[:, None, :]
    turned = jnp.stack([even_part * cos_tab - odd_part * sin_tab, even_part * sin_tab + odd_part * cos_tab], axis=-1)
    return turned.reshape(vecs.shape)


def reference(x, seq_lens, w_query, w_key, w_value, w_out, w_gate, w_up, w_down, attn_gain, mlp_gain, k_cache, v_cache):
    group_size = HEADS // KV_HEADS
    heads_part = HEADS * HEAD // TP
    ff_part = FF // TP
    positions = jnp.arange(SEQ)
    inv_freq = ROPE_BASE ** (-jnp.arange(0, HEAD, 2).astype(jnp.float32) / HEAD)
    angles = positions.astype(jnp.float32)[:, None] * inv_freq[None, :]
    causal = positions[None, :] <= positions[:, None]

    def one_sequence(items):
        x_row, length = items
        normed = rms_norm(x_row, attn_gain)
        queries = rotary(jnp.dot(normed, w_query, preferred_element_type=jnp.float32).reshape(SEQ, HEADS, HEAD), angles).astype(jnp.bfloat16)
        keys = rotary(jnp.dot(normed, w_key, preferred_element_type=jnp.float32).reshape(SEQ, KV_HEADS, HEAD), angles).astype(jnp.bfloat16)
        values = jnp.dot(normed, w_value, preferred_element_type=jnp.float32).astype(jnp.bfloat16).reshape(SEQ, KV_HEADS, HEAD)
        valid = positions < length
        keys = jnp.where(valid[:, None, None], keys, jnp.zeros_like(keys))
        values = jnp.where(valid[:, None, None], values, jnp.zeros_like(values))
        allowed = causal & valid[None, :]

        def one_kv_head(blocks):
            q_block, k_block, v_block = blocks
            scores = jnp.einsum("qgh,sh->gqs", q_block.astype(jnp.float32), k_block.astype(jnp.float32)) * HEAD ** -0.5
            scores = jnp.where(allowed[None], scores, -jnp.inf)
            probs = jax.nn.softmax(scores, axis=-1).astype(jnp.bfloat16)
            mixed = jnp.einsum("gqs,sh->qgh", probs.astype(jnp.float32), v_block.astype(jnp.float32))
            return mixed.astype(jnp.bfloat16)

        q_grouped = jnp.transpose(queries.reshape(SEQ, KV_HEADS, group_size, HEAD), (1, 0, 2, 3))
        head_out = lax.map(one_kv_head, (q_grouped, jnp.transpose(keys, (1, 0, 2)), jnp.transpose(values, (1, 0, 2))))
        attn_rows = jnp.transpose(head_out, (1, 0, 2, 3)).reshape(SEQ, HEADS * HEAD)
        attn_sum = jnp.zeros((SEQ, D), jnp.float32)
        for index in range(TP):
            partial = jnp.dot(attn_rows[:, index * heads_part:(index + 1) * heads_part], w_out[index * heads_part:(index + 1) * heads_part], preferred_element_type=jnp.float32)
            attn_sum = attn_sum + partial.astype(jnp.bfloat16).astype(jnp.float32)
        hidden = (x_row.astype(jnp.float32) + attn_sum).astype(jnp.bfloat16)
        normed_mlp = rms_norm(hidden, mlp_gain)
        gate_pre = jnp.dot(normed_mlp, w_gate, preferred_element_type=jnp.float32)
        up_pre = jnp.dot(normed_mlp, w_up, preferred_element_type=jnp.float32)
        gated = (jax.nn.silu(gate_pre) * up_pre).astype(jnp.bfloat16)
        mlp_sum = jnp.zeros((SEQ, D), jnp.float32)
        for index in range(TP):
            partial = jnp.dot(gated[:, index * ff_part:(index + 1) * ff_part], w_down[index * ff_part:(index + 1) * ff_part], preferred_element_type=jnp.float32)
            mlp_sum = mlp_sum + partial.astype(jnp.bfloat16).astype(jnp.float32)
        out_row = (hidden.astype(jnp.float32) + mlp_sum).astype(jnp.bfloat16)
        return out_row, keys, values

    y, new_keys, new_values = lax.map(one_sequence, (x, seq_lens))
    k_cache_out = lax.dynamic_update_slice(k_cache, new_keys, (0, 0, 0, 0))
    v_cache_out = lax.dynamic_update_slice(v_cache, new_values, (0, 0, 0, 0))
    return y, k_cache_out, v_cache_out
```

```python
import functools

import jax
import jax.numpy as jnp
from jax import lax
from jax.experimental import pallas as pl
from jax.experimental.pallas import tpu as pltpu
from jax.sharding import PartitionSpec as P


EPS = 1e-5
ROPE_BASE = 10000.0
CHUNKS = (1, 2, 2, 2, 1)
F32 = jnp.float32
BF16 = jnp.bfloat16
ANY = pl.BlockSpec(memory_space=pl.ANY)


def rope_tables(seq_len, head_dim):
    inv_freq = ROPE_BASE ** (-jnp.arange(0, head_dim, 2).astype(F32) / head_dim)
    angles = jnp.arange(seq_len).astype(F32)[:, None] * inv_freq[None, :]
    cos_tab = jnp.repeat(jnp.cos(angles), 2, axis=1)
    sin_tab = jnp.sin(angles)
    sin_tab = jnp.stack([-sin_tab, sin_tab], axis=-1).reshape(seq_len, head_dim)
    return cos_tab, sin_tab


def turn(vecs, cos_tab, sin_tab, even_lane):
    width = vecs.shape[1]
    swapped = jnp.where(even_lane, pltpu.roll(vecs, width - 1, 1), pltpu.roll(vecs, 1, 1))
    return vecs * cos_tab + swapped * sin_tab


def attention_kernel(first_seq, group_size, head_dim, lens_ref, q_ref, k_ref, v_ref, cos_ref, sin_ref, o_ref, k_out_ref, v_out_ref):
    seq_len = q_ref.shape[0]
    length = lens_ref[first_seq + pl.program_id(0)]
    cos_tab = cos_ref[...]
    sin_tab = sin_ref[...]
    even_lane = lax.broadcasted_iota(jnp.int32, (seq_len, head_dim), 1) % 2 == 0
    valid = lax.broadcasted_iota(jnp.int32, (seq_len, head_dim), 0) < length
    keys = jnp.where(valid, turn(k_ref[...], cos_tab, sin_tab, even_lane), 0.0).astype(BF16)
    values = jnp.where(valid, v_ref[...], 0.0).astype(BF16)
    k_out_ref[...] = keys
    v_out_ref[...] = values
    step = 128
    for head in range(group_size):
        cols = slice(head * head_dim, (head + 1) * head_dim)
        queries = turn(q_ref[:, cols], cos_tab, sin_tab, even_lane).astype(BF16)
        for start in range(0, seq_len, step):
            stop = start + step
            scores = lax.dot_general(queries[start:stop], keys[:stop], (((1,), (1,)), ((), ())), preferred_element_type=F32) * head_dim ** -0.5
            row = lax.broadcasted_iota(jnp.int32, (step, stop), 0) + start
            col = lax.broadcasted_iota(jnp.int32, (step, stop), 1)
            scores = jnp.where((col <= row) & (col < length), scores, -jnp.inf)
            exps = jnp.exp(scores - jnp.max(scores, axis=1, keepdims=True))
            probs = (exps / jnp.sum(exps, axis=1, keepdims=True)).astype(BF16)
            o_ref[start:stop, cols] = jnp.dot(probs, values[:stop], preferred_element_type=F32).astype(BF16)


def attention(lens, queries, kv, cos_tab, sin_tab, first_seq, n_seq, seq_len, head_dim):
    rows = n_seq * seq_len
    kv_local = kv.shape[1] // 2 // head_dim
    group_size = queries.shape[1] // (kv_local * head_dim)
    wide = group_size * head_dim
    per_head = pl.BlockSpec((seq_len, head_dim), lambda b, g, lens: (b, g))
    grouped = pl.BlockSpec((seq_len, wide), lambda b, g, lens: (b, g))
    table = pl.BlockSpec((seq_len, head_dim), lambda b, g, lens: (0, 0))
    return pl.pallas_call(
        functools.partial(attention_kernel, first_seq, group_size, head_dim),
        grid_spec=pltpu.PrefetchScalarGridSpec(
            num_scalar_prefetch=1,
            grid=(n_seq, kv_local),
            in_specs=[grouped, per_head, pl.BlockSpec((seq_len, head_dim), lambda b, g, lens: (b, kv_local + g)), table, table],
            out_specs=[grouped, per_head, per_head],
        ),
        out_shape=[
            jax.ShapeDtypeStruct((rows, queries.shape[1]), BF16),
            jax.ShapeDtypeStruct((rows, kv_local * head_dim), BF16),
            jax.ShapeDtypeStruct((rows, kv_local * head_dim), BF16),
        ],
        cost_estimate=pl.CostEstimate(flops=16 * rows * queries.shape[1] * seq_len, bytes_accessed=rows * queries.shape[1] * 8, transcendentals=rows * seq_len * group_size * kv_local),
        name="attention",
    )(lens, queries, kv, kv, cos_tab, sin_tab)


def rows_norm_kernel(x_ref, gain_ref, *rest):
    out_ref = rest[-1]
    x32 = x_ref[...].astype(F32)
    inv_rms = lax.rsqrt(jnp.mean(x32 * x32, axis=-1, keepdims=True) + EPS)
    out_ref[...] = (x32 * inv_rms * gain_ref[...]).astype(BF16)


def rows_norm(x_rows, gain, first_row, rows, deps):
    width = x_rows.shape[1]
    block = 128
    return pl.pallas_call(
        rows_norm_kernel,
        grid=(rows // block,),
        in_specs=[pl.BlockSpec((block, width), lambda i: (first_row // block + i, 0)), pl.BlockSpec((1, width), lambda i: (0, 0))] + [ANY] * len(deps),
        out_specs=pl.BlockSpec((block, width), lambda i: (i, 0)),
        out_shape=jax.ShapeDtypeStruct((rows, width), BF16),
        cost_estimate=pl.CostEstimate(flops=rows * width * 400, bytes_accessed=rows * width * 4, transcendentals=0),
        name="rows_norm",
    )(x_rows, gain, *deps)


def hidden_norm_kernel(h_ref, gain_ref, *rest):
    out_ref = rest[-1]
    parts, _, cols = h_ref.shape
    total = 0.0
    for part in range(parts):
        h32 = h_ref[part].astype(F32)
        total = total + jnp.sum(h32 * h32, axis=-1, keepdims=True)
    inv_rms = lax.rsqrt(total / (parts * cols) + EPS)
    for part in range(parts):
        span = slice(part * cols, (part + 1) * cols)
        out_ref[:, span] = (h_ref[part].astype(F32) * inv_rms * gain_ref[:, span]).astype(BF16)


def hidden_norm(hidden, gain, deps):
    parts, rows, cols = hidden.shape
    block = 128
    width = parts * cols
    return pl.pallas_call(
        hidden_norm_kernel,
        grid=(rows // block,),
        in_specs=[pl.BlockSpec((parts, block, cols), lambda i: (0, i, 0)), pl.BlockSpec((1, width), lambda i: (0, 0))] + [ANY] * len(deps),
        out_specs=pl.BlockSpec((block, width), lambda i: (i, 0)),
        out_shape=jax.ShapeDtypeStruct((rows, width), BF16),
        cost_estimate=pl.CostEstimate(flops=rows * width * 400, bytes_accessed=rows * width * 4, transcendentals=0),
        name="hidden_norm",
    )(hidden, gain, *deps)


def out_proj_kernel(n_far, place_ref, heads_ref, x_ref, own_ref, near_ref, *rest):
    far_refs, h_ref = rest[:n_far], rest[-1]
    tp_index, dp_index = place_ref[0], place_ref[1]
    total = x_ref[...].astype(F32)
    half = far_refs[0].shape[0]
    for hop, block in enumerate((own_ref, near_ref)):
        total = total + jnp.dot(heads_ref[tp_index ^ hop], block[...], preferred_element_type=F32).astype(BF16).astype(F32)
    for hop in range(2, 2 + len(far_refs) // 2):
        part = 0.0
        for side in range(2):
            start = pl.multiple_of((dp_index ^ side) * half, half)
            part = part + jnp.dot(heads_ref[tp_index ^ hop, :, pl.ds(start, half)], far_refs[2 * (hop - 2) + side][...], preferred_element_type=F32)
        total = total + part.astype(BF16).astype(F32)
    h_ref[...] = total.astype(BF16)


def out_proj(place, heads, x_rows, w_out, near, far, first_row, deps):
    parts, rows, width = heads.shape
    cols = near.shape[1]
    block = 256
    steps = cols // block
    half = far[0].shape[0]
    return pl.pallas_call(
        functools.partial(out_proj_kernel, len(far)),
        grid_spec=pltpu.PrefetchScalarGridSpec(
            num_scalar_prefetch=1,
            grid=(steps,),
            in_specs=[
                pl.BlockSpec((parts, rows, width), lambda n, place: (0, 0, 0)),
                pl.BlockSpec((rows, block), lambda n, place: (first_row // rows, place[0] * steps + n)) if first_row % rows == 0 else pl.BlockSpec((pl.Element(rows), pl.Element(block)), lambda n, place: (first_row, (place[0] * steps + n) * block)),
                pl.BlockSpec((width, block), lambda n, place: (0, place[0] * steps + n)),
                pl.BlockSpec((width, block), lambda n, place: (0, n)),
            ] + [pl.BlockSpec((half, block), lambda n, place: (0, n))] * len(far) + [ANY] * len(deps),
            out_specs=pl.BlockSpec((rows, block), lambda n, place: (0, n)),
        ),
        out_shape=jax.ShapeDtypeStruct((rows, cols), BF16),
        compiler_params=pltpu.CompilerParams(vmem_limit_bytes=56 * 2**20),
        cost_estimate=pl.CostEstimate(flops=2 * parts * rows * width * cols, bytes_accessed=parts * (rows + cols) * width * 2, transcendentals=0),
        name="out_proj",
    )(place, heads, x_rows, w_out, near, *far, *deps)


def sum_kernel(place_ref, received_ref, h_ref, *rest):
    out_ref = rest[-1]
    parts, _, cols = h_ref.shape
    for part in range(parts):
        span = slice(part * cols, (part + 1) * cols)
        total = received_ref[0, :, span].astype(F32)
        for source in range(1, parts):
            total = total + received_ref[source, :, span].astype(F32)
        out_ref[:, span] = (h_ref[part].astype(F32) + total).astype(BF16)


def sum_rows(place, received, hidden, deps):
    parts, rows, width = received.shape
    cols = hidden.shape[2]
    block = 48
    steps = rows // block
    return pl.pallas_call(
        sum_kernel,
        grid_spec=pltpu.PrefetchScalarGridSpec(
            num_scalar_prefetch=1,
            grid=(steps,),
            in_specs=[
                pl.BlockSpec((parts, block, width), lambda i, place: (0, i, 0)),
                pl.BlockSpec((parts, block, cols), lambda i, place: (0, place[0] * steps + i, 0)),
            ] + [ANY] * len(deps),
            out_specs=pl.BlockSpec((block, width), lambda i, place: (i, 0)),
        ),
        out_shape=jax.ShapeDtypeStruct((rows, width), BF16),
        cost_estimate=pl.CostEstimate(flops=rows * width * 600, bytes_accessed=rows * width * 12, transcendentals=0),
        name="sum_rows",
    )(place, received, hidden, *deps)


def store_kernel(*refs):
    refs[-1][...] = refs[0][...]


def store_rows(y, y_part, first_row, total_rows, deps):
    rows, width = y_part.shape
    block = 128
    return pl.pallas_call(
        store_kernel,
        grid=(rows // block,),
        in_specs=[pl.BlockSpec((block, width), lambda i: (i, 0))] + [ANY] * (len(deps) + (y is not None)),
        out_specs=pl.BlockSpec((block, width), lambda i: (first_row // block + i, 0)),
        out_shape=jax.ShapeDtypeStruct((total_rows, width), BF16),
        input_output_aliases={} if y is None else {1: 0},
        cost_estimate=pl.CostEstimate(flops=rows * width * 300, bytes_accessed=rows * width * 4, transcendentals=0),
        name="store_rows",
    )(*([y_part] if y is None else [y_part, y]), *deps)


def solution(mesh):
    tp_size = mesh.shape["tp"]
    dp_size = mesh.shape["dp"]

    def layer_shard(x, seq_lens, w_query, w_key, w_value, w_out, w_gate, w_up, w_down, attn_gain, mlp_gain, k_cache, v_cache):
        batch_size, seq_len, width = x.shape
        kv_local, head_dim = k_cache.shape[2:]
        q_width = w_query.shape[1]
        tp_index = lax.axis_index("tp")
        dp_index = lax.axis_index("dp")
        place = jnp.stack([tp_index, dp_index]).astype(jnp.int32)
        part_cols = width // tp_size
        total_rows = batch_size * seq_len
        x_rows = x.reshape(total_rows, width)
        chunks = len(CHUNKS)
        first = [sum(CHUNKS[:c]) for c in range(chunks)]

        half = q_width // dp_size
        swaps = [[(i, i ^ hop) for i in range(tp_size)] for hop in range(tp_size)]
        dp_ring = [(i, (i + 1) % dp_size) for i in range(dp_size)]
        mine = []
        other = []
        for hop in range(2, tp_size):
            block = lax.dynamic_slice(w_out, (dp_index * half, (tp_index ^ hop) * part_cols), (half, part_cols))
            mine.append(lax.ppermute(block, "tp", swaps[hop]))
            other.append(lax.ppermute(mine[-1], "dp", dp_ring))
        block = lax.dynamic_slice_in_dim(w_out, (tp_index ^ 1) * part_cols, part_cols, axis=1)
        near = lax.ppermute(block, "tp", swaps[1])

        w_kv = jnp.concatenate([w_key, w_value], axis=1)
        cos_tab, sin_tab = rope_tables(seq_len, head_dim)
        gain = attn_gain.astype(F32).reshape(1, width)
        mlp_gain32 = mlp_gain.astype(F32).reshape(1, width)

        heads = []
        new_keys = []
        new_values = []
        deps = []
        for c in range(chunks):
            rows = CHUNKS[c] * seq_len
            if c >= 3:
                deps = deps + [mine[c - 3]]
            normed = rows_norm(x_rows, gain, first[c] * seq_len, rows, deps)
            queries = jnp.dot(normed, w_query, preferred_element_type=F32)
            kv = jnp.dot(normed, w_kv, preferred_element_type=F32)
            out, keys, values = attention(seq_lens, queries, kv, cos_tab, sin_tab, first[c], CHUNKS[c], seq_len, head_dim)
            deps = [out]
            heads.append(lax.all_gather(out, "tp", axis=0))
            new_keys.append(keys)
            new_values.append(values)

        hidden = {}
        received = {}
        gathered = {}
        y = None

        def project(c, deps):
            local = out_proj(place, heads[c], x_rows, w_out, near, [mine[0], other[0], mine[1], other[1]], first[c] * seq_len, deps)
            hidden[c] = lax.all_gather(local, "tp", axis=0)
            return [local]

        def finish(c, deps):
            y_rows = sum_rows(place, received[c], hidden[c], deps)
            gathered[c] = lax.all_gather(y_rows, "tp", axis=0, tiled=True)
            return [y_rows]

        def store(c, y, deps):
            return store_rows(y, gathered[c], first[c] * seq_len, total_rows, deps)

        deps = project(0, deps)
        deps = project(1, deps)
        for c in range(chunks):
            rows = CHUNKS[c] * seq_len
            normed = hidden_norm(hidden[c], mlp_gain32, deps)
            gate = lax.optimization_barrier(jnp.dot(normed, w_gate, preferred_element_type=F32))
            up = jnp.dot(normed, w_up, preferred_element_type=F32)
            gated = lax.optimization_barrier((jax.nn.silu(gate) * up).astype(BF16))
            part = jnp.dot(gated, w_down, preferred_element_type=F32).astype(BF16)
            received[c] = lax.all_to_all(part.reshape(tp_size, rows // tp_size, width), "tp", 0, 0, tiled=True)
            deps = [part]
            if c >= 1:
                deps = finish(c - 1, deps)
            if c >= 2:
                y = store(c - 2, y, deps)
                deps = [y]
            if c + 2 < chunks:
                deps = project(c + 2, deps)
        y = store(chunks - 2, y, [])
        finish(chunks - 1, [])
        y = store(chunks - 1, y, [])

        def cache(old, new):
            new = jnp.concatenate(new, axis=0).reshape(batch_size, seq_len, kv_local, head_dim)
            return lax.dynamic_update_slice(old, new, (0, 0, 0, 0))

        return y.reshape(x.shape), cache(k_cache, new_keys), cache(v_cache, new_values)

    cache_spec = P("dp", None, "tp", None)
    return jax.shard_map(layer_shard, mesh=mesh, in_specs=(P("dp", None, None), P("dp"), P(None, "tp"), P(None, "tp"), P(None, "tp"), P("tp", None), P(None, "tp"), P(None, "tp"), P("tp", None), P(), P(), cache_spec, cache_spec), out_specs=(P("dp", None, None), cache_spec, cache_spec), check_vma=False)
```

```python
import functools

import jax
import jax.numpy as jnp
from jax import lax
from jax.experimental import pallas as pl
from jax.experimental.pallas import tpu as pltpu
from jax.sharding import PartitionSpec as P


EPS = 1e-5
ROPE_BASE = 10000.0
CHUNKS = (1, 2, 2, 2, 1)
F32 = jnp.float32
BF16 = jnp.bfloat16
ANY = pl.BlockSpec(memory_space=pl.ANY)


def rope_tables(seq_len, head_dim):
    inv_freq = ROPE_BASE ** (-jnp.arange(0, head_dim, 2).astype(F32) / head_dim)
    angles = jnp.arange(seq_len).astype(F32)[:, None] * inv_freq[None, :]
    cos_tab = jnp.repeat(jnp.cos(angles), 2, axis=1)
    sin_tab = jnp.sin(angles)
    sin_tab = jnp.stack([-sin_tab, sin_tab], axis=-1).reshape(seq_len, head_dim)
    return cos_tab, sin_tab


def turn(vecs, cos_tab, sin_tab, even_lane):
    width = vecs.shape[1]
    swapped = jnp.where(even_lane, pltpu.roll(vecs, width - 1, 1), pltpu.roll(vecs, 1, 1))
    return vecs * cos_tab + swapped * sin_tab


def attention_kernel(first_seq, group_size, head_dim, lens_ref, q_ref, k_ref, v_ref, cos_ref, sin_ref, o_ref, k_out_ref, v_out_ref):
    seq_len = q_ref.shape[0]
    length = lens_ref[first_seq + pl.program_id(0)]
    cos_tab = cos_ref[...]
    sin_tab = sin_ref[...]
    even_lane = lax.broadcasted_iota(jnp.int32, (seq_len, head_dim), 1) % 2 == 0
    valid = lax.broadcasted_iota(jnp.int32, (seq_len, head_dim), 0) < length
    keys = jnp.where(valid, turn(k_ref[...], cos_tab, sin_tab, even_lane), 0.0).astype(BF16)
    values = jnp.where(valid, v_ref[...], 0.0).astype(BF16)
    k_out_ref[...] = keys
    v_out_ref[...] = values
    step = 128
    turned = []
    for head in range(group_size):
        cols = slice(head * head_dim, (head + 1) * head_dim)
        turned.append(turn(q_ref[:, cols], cos_tab, sin_tab, even_lane).astype(BF16))
    factor = head_dim ** -0.5 * 1.4426950408889634
    for start in range(0, seq_len, step):
        stop = start + step
        queries = jnp.concatenate([head[start:stop] for head in turned], axis=0)
        scores = lax.dot_general(queries, keys[:stop], (((1,), (1,)), ((), ())), preferred_element_type=F32)
        row = lax.broadcasted_iota(jnp.int32, (step, stop), 0) + start
        col = lax.broadcasted_iota(jnp.int32, (step, stop), 1)
        hide = jnp.where((col <= row) & (col < length), 0.0, -jnp.inf)
        scores = scores.reshape(group_size, step, stop) + hide[None]
        exps = jnp.exp2((scores - jnp.max(scores, axis=2, keepdims=True)) * factor)
        probs = (exps * (1.0 / jnp.sum(exps, axis=2, keepdims=True))).astype(BF16)
        mixed = jnp.dot(probs.reshape(group_size * step, stop), values[:stop], preferred_element_type=F32).astype(BF16)
        for head in range(group_size):
            o_ref[start:stop, head * head_dim:(head + 1) * head_dim] = mixed[head * step:(head + 1) * step]


def attention(lens, qkv, cos_tab, sin_tab, first_seq, n_seq, seq_len, head_dim, kv_local):
    rows = n_seq * seq_len
    heads = qkv.shape[1] // head_dim - 2 * kv_local
    group_size = heads // kv_local
    wide = group_size * head_dim
    per_head = [pl.BlockSpec((seq_len, head_dim), functools.partial(lambda offset, b, g, lens: (b, offset + g), offset)) for offset in (heads, heads + kv_local, 0)]
    grouped = pl.BlockSpec((seq_len, wide), lambda b, g, lens: (b, g))
    table = pl.BlockSpec((seq_len, head_dim), lambda b, g, lens: (0, 0))
    return pl.pallas_call(
        functools.partial(attention_kernel, first_seq, group_size, head_dim),
        grid_spec=pltpu.PrefetchScalarGridSpec(
            num_scalar_prefetch=1,
            grid=(n_seq, kv_local),
            in_specs=[grouped, per_head[0], per_head[1], table, table],
            out_specs=[grouped, per_head[2], per_head[2]],
        ),
        out_shape=[
            jax.ShapeDtypeStruct((rows, heads * head_dim), BF16),
            jax.ShapeDtypeStruct((rows, kv_local * head_dim), BF16),
            jax.ShapeDtypeStruct((rows, kv_local * head_dim), BF16),
        ],
        cost_estimate=pl.CostEstimate(flops=16 * rows * heads * head_dim * seq_len, bytes_accessed=rows * heads * head_dim * 8, transcendentals=rows * seq_len * heads),
        name="attention",
    )(lens, qkv, qkv, qkv, cos_tab, sin_tab)


NORM_ROWS = 128
NORM_COLS = 512
TILE = 256


def inv_rms_of(parts):
    total = 0.0
    width = 0
    for part in parts:
        for start in range(0, part.shape[1], NORM_COLS // 2):
            x32 = part[:, start:start + NORM_COLS // 2].astype(F32)
            square = x32 * x32
            for lane in range(0, square.shape[1], 128):
                total = total + square[:, lane:lane + 128]
        width += part.shape[1]
    return lax.rsqrt(jnp.sum(total, axis=1, keepdims=True) / width + EPS)


def norm_into(parts, gain_ref, normed_ref, row):
    inv_rms = inv_rms_of(parts)
    column = 0
    for part in parts:
        for start in range(0, part.shape[1], NORM_COLS // 2):
            span = slice(column, column + NORM_COLS // 2)
            normed_ref[pl.ds(row, part.shape[0]), span] = (part[:, start:start + NORM_COLS // 2].astype(F32) * inv_rms * gain_ref[:, span]).astype(BF16)
            column += NORM_COLS // 2


def qkv_kernel(steps, q_tiles, x_ref, gain_ref, wq_ref, wkv_ref, *rest):
    out_ref, normed_ref = rest[-2:]
    i = pl.program_id(0)

    @pl.when(i < steps)
    def _():
        norm_into([x_ref], gain_ref, normed_ref, pl.multiple_of(i * NORM_ROWS, NORM_ROWS))

    @pl.when((i >= steps) & (i < steps + q_tiles))
    def _():
        out_ref[...] = jnp.dot(normed_ref[...], wq_ref[...], preferred_element_type=F32)

    @pl.when(i >= steps + q_tiles)
    def _():
        out_ref[...] = jnp.dot(normed_ref[...], wkv_ref[...], preferred_element_type=F32)


def qkv_proj(x_rows, gain, w_query, w_kv, first_row, rows, deps):
    width = x_rows.shape[1]
    steps = rows // NORM_ROWS
    q_tiles = w_query.shape[1] // TILE
    kv_tiles = w_kv.shape[1] // TILE
    cols = w_query.shape[1] + w_kv.shape[1]
    return pl.pallas_call(
        functools.partial(qkv_kernel, steps, q_tiles),
        grid=(steps + q_tiles + kv_tiles,),
        in_specs=[
            pl.BlockSpec((NORM_ROWS, width), lambda i: (first_row // NORM_ROWS + jnp.minimum(i, steps - 1), 0)),
            pl.BlockSpec((1, width), lambda i: (0, 0)),
            pl.BlockSpec((width, TILE), lambda i: (0, jnp.clip(i - steps, 0, q_tiles - 1))),
            pl.BlockSpec((width, TILE), lambda i: (0, jnp.clip(i - steps - q_tiles, 0, kv_tiles - 1))),
        ] + [ANY] * len(deps),
        out_specs=pl.BlockSpec((rows, TILE), lambda i: (0, jnp.maximum(i - steps, 0))),
        out_shape=jax.ShapeDtypeStruct((rows, cols), F32),
        scratch_shapes=[pltpu.VMEM((rows, width), BF16)],
        compiler_params=pltpu.CompilerParams(vmem_limit_bytes=50 * 2**20),
        cost_estimate=pl.CostEstimate(flops=2 * rows * width * cols, bytes_accessed=width * cols * 2 + rows * width * 2 + rows * cols * 4, transcendentals=0),
        name="qkv_proj",
    )(x_rows, gain, w_query, w_kv, *deps)


def gated_kernel(steps, h_ref, gain_ref, gate_ref, up_ref, *rest):
    out_ref, normed_ref = rest[-2:]
    i = pl.program_id(0)

    @pl.when(i < steps)
    def _():
        norm_into([h_ref.at[part] for part in range(h_ref.shape[0])], gain_ref, normed_ref, pl.multiple_of(i * NORM_ROWS, NORM_ROWS))

    @pl.when(i >= steps)
    def _():
        gate = jnp.dot(normed_ref[...], gate_ref[...], preferred_element_type=F32)
        up = jnp.dot(normed_ref[...], up_ref[...], preferred_element_type=F32)
        out_ref[...] = (jax.nn.silu(gate) * up).astype(BF16)


def gated_proj(hidden, gain, w_gate, w_up, deps):
    parts, rows, part_cols = hidden.shape
    width, cols = w_gate.shape
    steps = rows // NORM_ROWS
    weight = pl.BlockSpec((width, TILE), lambda i: (0, jnp.maximum(i - steps, 0)))
    return pl.pallas_call(
        functools.partial(gated_kernel, steps),
        grid=(steps + cols // TILE,),
        in_specs=[
            pl.BlockSpec((parts, NORM_ROWS, part_cols), lambda i: (0, jnp.minimum(i, steps - 1), 0)),
            pl.BlockSpec((1, width), lambda i: (0, 0)),
            weight,
            weight,
        ] + [ANY] * len(deps),
        out_specs=pl.BlockSpec((rows, TILE), lambda i: (0, jnp.maximum(i - steps, 0))),
        out_shape=jax.ShapeDtypeStruct((rows, cols), BF16),
        scratch_shapes=[pltpu.VMEM((rows, width), BF16)],
        compiler_params=pltpu.CompilerParams(vmem_limit_bytes=50 * 2**20),
        cost_estimate=pl.CostEstimate(flops=4 * rows * width * cols, bytes_accessed=width * cols * 4 + rows * width * 2 + rows * cols * 2, transcendentals=rows * cols),
        name="gated_proj",
    )(hidden, gain, w_gate, w_up, *deps)


def out_proj_kernel(n_far, place_ref, heads_ref, x_ref, own_ref, near_ref, *rest):
    far_refs, h_ref = rest[:n_far], rest[-1]
    tp_index, dp_index = place_ref[0], place_ref[1]
    total = x_ref[...].astype(F32)
    half = far_refs[0].shape[0]
    for hop, block in enumerate((own_ref, near_ref)):
        total = total + jnp.dot(heads_ref[tp_index ^ hop], block[...], preferred_element_type=F32).astype(BF16).astype(F32)
    for hop in range(2, 2 + len(far_refs) // 2):
        part = 0.0
        for side in range(2):
            start = pl.multiple_of((dp_index ^ side) * half, half)
            part = part + jnp.dot(heads_ref[tp_index ^ hop, :, pl.ds(start, half)], far_refs[2 * (hop - 2) + side][...], preferred_element_type=F32)
        total = total + part.astype(BF16).astype(F32)
    h_ref[...] = total.astype(BF16)


def out_proj(place, heads, x_rows, w_out, near, far, first_row, deps):
    parts, rows, width = heads.shape
    cols = near.shape[1]
    block = 256
    steps = cols // block
    half = far[0].shape[0]
    return pl.pallas_call(
        functools.partial(out_proj_kernel, len(far)),
        grid_spec=pltpu.PrefetchScalarGridSpec(
            num_scalar_prefetch=1,
            grid=(steps,),
            in_specs=[
                pl.BlockSpec((parts, rows, width), lambda n, place: (0, 0, 0)),
                pl.BlockSpec((rows, block), lambda n, place: (first_row // rows, place[0] * steps + n)) if first_row % rows == 0 else pl.BlockSpec((pl.Element(rows), pl.Element(block)), lambda n, place: (first_row, (place[0] * steps + n) * block)),
                pl.BlockSpec((width, block), lambda n, place: (0, place[0] * steps + n)),
                pl.BlockSpec((width, block), lambda n, place: (0, n)),
            ] + [pl.BlockSpec((half, block), lambda n, place: (0, n))] * len(far) + [ANY] * len(deps),
            out_specs=pl.BlockSpec((rows, block), lambda n, place: (0, n)),
        ),
        out_shape=jax.ShapeDtypeStruct((rows, cols), BF16),
        compiler_params=pltpu.CompilerParams(vmem_limit_bytes=56 * 2**20),
        cost_estimate=pl.CostEstimate(flops=2 * parts * rows * width * cols, bytes_accessed=parts * (rows + cols) * width * 2, transcendentals=0),
        name="out_proj",
    )(place, heads, x_rows, w_out, near, *far, *deps)


def sum_kernel(place_ref, received_ref, h_ref, *rest):
    out_ref = rest[-1]
    parts, _, cols = h_ref.shape
    for part in range(parts):
        span = slice(part * cols, (part + 1) * cols)
        total = received_ref[0, :, span].astype(F32)
        for source in range(1, parts):
            total = total + received_ref[source, :, span].astype(F32)
        out_ref[:, span] = (h_ref[part].astype(F32) + total).astype(BF16)


def sum_rows(place, received, hidden, deps):
    parts, rows, width = received.shape
    cols = hidden.shape[2]
    block = 48
    steps = rows // block
    return pl.pallas_call(
        sum_kernel,
        grid_spec=pltpu.PrefetchScalarGridSpec(
            num_scalar_prefetch=1,
            grid=(steps,),
            in_specs=[
                pl.BlockSpec((parts, block, width), lambda i, place: (0, i, 0)),
                pl.BlockSpec((parts, block, cols), lambda i, place: (0, place[0] * steps + i, 0)),
            ] + [ANY] * len(deps),
            out_specs=pl.BlockSpec((block, width), lambda i, place: (i, 0)),
        ),
        out_shape=jax.ShapeDtypeStruct((rows, width), BF16),
        cost_estimate=pl.CostEstimate(flops=rows * width * 600, bytes_accessed=rows * width * 12, transcendentals=0),
        name="sum_rows",
    )(place, received, hidden, *deps)


def store_kernel(*refs):
    refs[-1][...] = refs[0][...]


def store_rows(y, y_part, first_row, total_rows, deps):
    rows, width = y_part.shape
    block = 128
    return pl.pallas_call(
        store_kernel,
        grid=(rows // block,),
        in_specs=[pl.BlockSpec((block, width), lambda i: (i, 0))] + [ANY] * (len(deps) + (y is not None)),
        out_specs=pl.BlockSpec((block, width), lambda i: (first_row // block + i, 0)),
        out_shape=jax.ShapeDtypeStruct((total_rows, width), BF16),
        input_output_aliases={} if y is None else {1: 0},
        cost_estimate=pl.CostEstimate(flops=rows * width * 300, bytes_accessed=rows * width * 4, transcendentals=0),
        name="store_rows",
    )(*([y_part] if y is None else [y_part, y]), *deps)


def solution(mesh):
    tp_size = mesh.shape["tp"]
    dp_size = mesh.shape["dp"]

    def layer_shard(x, seq_lens, w_query, w_key, w_value, w_out, w_gate, w_up, w_down, attn_gain, mlp_gain, k_cache, v_cache):
        batch_size, seq_len, width = x.shape
        kv_local, head_dim = k_cache.shape[2:]
        q_width = w_query.shape[1]
        tp_index = lax.axis_index("tp")
        dp_index = lax.axis_index("dp")
        place = jnp.stack([tp_index, dp_index]).astype(jnp.int32)
        part_cols = width // tp_size
        total_rows = batch_size * seq_len
        x_rows = x.reshape(total_rows, width)
        chunks = len(CHUNKS)
        first = [sum(CHUNKS[:c]) for c in range(chunks)]

        half = q_width // dp_size
        swaps = [[(i, i ^ hop) for i in range(tp_size)] for hop in range(tp_size)]
        dp_ring = [(i, (i + 1) % dp_size) for i in range(dp_size)]
        mine = []
        other = []
        for hop in range(2, tp_size):
            block = lax.dynamic_slice(w_out, (dp_index * half, (tp_index ^ hop) * part_cols), (half, part_cols))
            mine.append(lax.ppermute(block, "tp", swaps[hop]))
            other.append(lax.ppermute(mine[-1], "dp", dp_ring))
        block = lax.dynamic_slice_in_dim(w_out, (tp_index ^ 1) * part_cols, part_cols, axis=1)
        near = lax.ppermute(block, "tp", swaps[1])

        w_kv = jnp.concatenate([w_key, w_value], axis=1)
        cos_tab, sin_tab = rope_tables(seq_len, head_dim)
        gain = attn_gain.astype(F32).reshape(1, width)
        mlp_gain32 = mlp_gain.astype(F32).reshape(1, width)

        heads = []
        new_keys = []
        new_values = []
        deps = []
        for c in range(chunks):
            rows = CHUNKS[c] * seq_len
            if c >= 3:
                deps = deps + [mine[c - 3]]
            qkv = qkv_proj(x_rows, gain, w_query, w_kv, first[c] * seq_len, rows, deps)
            out, keys, values = attention(seq_lens, qkv, cos_tab, sin_tab, first[c], CHUNKS[c], seq_len, head_dim, kv_local)
            deps = [out]
            heads.append(lax.all_gather(out, "tp", axis=0))
            new_keys.append(keys)
            new_values.append(values)

        hidden = {}
        received = {}
        gathered = {}
        y = None

        def project(c, deps):
            local = out_proj(place, heads[c], x_rows, w_out, near, [mine[0], other[0], mine[1], other[1]], first[c] * seq_len, deps)
            hidden[c] = lax.all_gather(local, "tp", axis=0)
            return [local]

        def finish(c, deps):
            y_rows = sum_rows(place, received[c], hidden[c], deps)
            gathered[c] = lax.all_gather(y_rows, "tp", axis=0, tiled=True)
            return [y_rows]

        def store(c, y, deps):
            return store_rows(y, gathered[c], first[c] * seq_len, total_rows, deps)

        deps = project(0, deps)
        deps = project(1, deps)
        for c in range(chunks):
            rows = CHUNKS[c] * seq_len
            gated = gated_proj(hidden[c], mlp_gain32, w_gate, w_up, deps)
            part = jnp.dot(gated, w_down, preferred_element_type=F32).astype(BF16)
            received[c] = lax.all_to_all(part.reshape(tp_size, rows // tp_size, width), "tp", 0, 0, tiled=True)
            deps = [part]
            if c >= 1:
                deps = finish(c - 1, deps)
            if c >= 2:
                y = store(c - 2, y, deps)
                deps = [y]
            if c + 2 < chunks:
                deps = project(c + 2, deps)
        y = store(chunks - 2, y, [])
        finish(chunks - 1, [])
        y = store(chunks - 1, y, [])

        def cache(old, new):
            new = jnp.concatenate(new, axis=0).reshape(batch_size, seq_len, kv_local, head_dim)
            return lax.dynamic_update_slice(old, new, (0, 0, 0, 0))

        return y.reshape(x.shape), cache(k_cache, new_keys), cache(v_cache, new_values)

    cache_spec = P("dp", None, "tp", None)
    return jax.shard_map(layer_shard, mesh=mesh, in_specs=(P("dp", None, None), P("dp"), P(None, "tp"), P(None, "tp"), P(None, "tp"), P("tp", None), P(None, "tp"), P(None, "tp"), P("tp", None), P(), P(), cache_spec, cache_spec), out_specs=(P("dp", None, None), cache_spec, cache_spec), check_vma=False)
```

```python
import functools

import jax
import jax.numpy as jnp
from jax import lax
from jax.experimental import pallas as pl
from jax.experimental.pallas import tpu as pltpu
from jax.sharding import PartitionSpec as P


EPS = 1e-5
ROPE_BASE = 10000.0
CHUNKS = (1, 2, 2, 2, 1)
F32 = jnp.float32
BF16 = jnp.bfloat16
ANY = pl.BlockSpec(memory_space=pltpu.MemorySpace.HBM)


def rope_tables(seq_len, head_dim):
    inv_freq = ROPE_BASE ** (-jnp.arange(0, head_dim, 2).astype(F32) / head_dim)
    angles = jnp.arange(seq_len).astype(F32)[:, None] * inv_freq[None, :]
    cos_tab = jnp.repeat(jnp.cos(angles), 2, axis=1)
    sin_tab = jnp.sin(angles)
    sin_tab = jnp.stack([-sin_tab, sin_tab], axis=-1).reshape(seq_len, head_dim)
    return cos_tab, sin_tab


def turn(vecs, cos_tab, sin_tab, even_lane):
    width = vecs.shape[1]
    swapped = jnp.where(even_lane, pltpu.roll(vecs, width - 1, 1), pltpu.roll(vecs, 1, 1))
    return vecs * cos_tab + swapped * sin_tab


def attention_kernel(first_seq, group_size, head_dim, lens_ref, q_ref, k_ref, v_ref, cos_ref, sin_ref, *rest):
    o_ref, k_out_ref, v_out_ref = rest[-3:]
    seq_len = q_ref.shape[0]
    length = lens_ref[first_seq + pl.program_id(0)]
    cos_tab = cos_ref[...]
    sin_tab = sin_ref[...]
    even_lane = lax.broadcasted_iota(jnp.int32, (seq_len, head_dim), 1) % 2 == 0
    valid = lax.broadcasted_iota(jnp.int32, (seq_len, head_dim), 0) < length
    keys = jnp.where(valid, turn(k_ref[...], cos_tab, sin_tab, even_lane), 0.0).astype(BF16)
    values = jnp.where(valid, v_ref[...], 0.0).astype(BF16)
    k_out_ref[...] = keys
    v_out_ref[...] = values
    step = 128
    turned = []
    for head in range(group_size):
        cols = slice(head * head_dim, (head + 1) * head_dim)
        turned.append(turn(q_ref[:, cols], cos_tab, sin_tab, even_lane).astype(BF16))
    factor = head_dim ** -0.5 * 1.4426950408889634
    for start in range(0, seq_len, step):
        stop = start + step
        queries = jnp.concatenate([head[start:stop] for head in turned], axis=0)
        scores = lax.dot_general(queries, keys[:stop], (((1,), (1,)), ((), ())), preferred_element_type=F32)
        row = lax.broadcasted_iota(jnp.int32, (step, stop), 0) + start
        col = lax.broadcasted_iota(jnp.int32, (step, stop), 1)
        hide = jnp.where((col <= row) & (col < length), 0.0, -jnp.inf)
        scores = scores.reshape(group_size, step, stop) + hide[None]
        exps = jnp.exp2((scores - jnp.max(scores, axis=2, keepdims=True)) * factor)
        probs = (exps * (1.0 / jnp.sum(exps, axis=2, keepdims=True))).astype(BF16)
        mixed = jnp.dot(probs.reshape(group_size * step, stop), values[:stop], preferred_element_type=F32).astype(BF16)
        for head in range(group_size):
            o_ref[start:stop, head * head_dim:(head + 1) * head_dim] = mixed[head * step:(head + 1) * step]


def attention(lens, qkv, cos_tab, sin_tab, first_seq, n_seq, seq_len, head_dim, kv_local, deps):
    rows = n_seq * seq_len
    heads = qkv.shape[1] // head_dim - 2 * kv_local
    group_size = heads // kv_local
    wide = group_size * head_dim
    per_head = [pl.BlockSpec((seq_len, head_dim), functools.partial(lambda offset, b, g, lens: (b, offset + g), offset)) for offset in (heads, heads + kv_local, 0)]
    grouped = pl.BlockSpec((seq_len, wide), lambda b, g, lens: (b, g))
    table = pl.BlockSpec((seq_len, head_dim), lambda b, g, lens: (0, 0))
    return pl.pallas_call(
        functools.partial(attention_kernel, first_seq, group_size, head_dim),
        grid_spec=pltpu.PrefetchScalarGridSpec(
            num_scalar_prefetch=1,
            grid=(n_seq, kv_local),
            in_specs=[grouped, per_head[0], per_head[1], table, table] + [ANY] * len(deps),
            out_specs=[grouped, per_head[2], per_head[2]],
        ),
        out_shape=[
            jax.ShapeDtypeStruct((rows, heads * head_dim), BF16),
            jax.ShapeDtypeStruct((rows, kv_local * head_dim), BF16),
            jax.ShapeDtypeStruct((rows, kv_local * head_dim), BF16),
        ],
        cost_estimate=pl.CostEstimate(flops=16 * rows * heads * head_dim * seq_len, bytes_accessed=rows * heads * head_dim * 8, transcendentals=rows * seq_len * heads),
        name="attention",
    )(lens, qkv, qkv, qkv, cos_tab, sin_tab, *deps)


NORM_ROWS = 128
NORM_COLS = 512
TILE = 256


def inv_rms_of(parts):
    total = 0.0
    width = 0
    for part in parts:
        for start in range(0, part.shape[1], NORM_COLS // 2):
            x32 = part[:, start:start + NORM_COLS // 2].astype(F32)
            square = x32 * x32
            for lane in range(0, square.shape[1], 128):
                total = total + square[:, lane:lane + 128]
        width += part.shape[1]
    return lax.rsqrt(jnp.sum(total, axis=1, keepdims=True) / width + EPS)


def norm_into(parts, gain_ref, normed_ref, row):
    inv_rms = inv_rms_of(parts)
    column = 0
    for part in parts:
        for start in range(0, part.shape[1], NORM_COLS // 2):
            span = slice(column, column + NORM_COLS // 2)
            normed_ref[pl.ds(row, part.shape[0]), span] = (part[:, start:start + NORM_COLS // 2].astype(F32) * inv_rms * gain_ref[:, span]).astype(BF16)
            column += NORM_COLS // 2


def qkv_kernel(steps, q_tiles, x_ref, gain_ref, wq_ref, wkv_ref, *rest):
    out_ref, normed_ref = rest[-2:]
    i = pl.program_id(0)

    @pl.when(i < steps)
    def _():
        norm_into([x_ref], gain_ref, normed_ref, pl.multiple_of(i * NORM_ROWS, NORM_ROWS))

    @pl.when((i >= steps) & (i < steps + q_tiles))
    def _():
        out_ref[...] = jnp.dot(normed_ref[...], wq_ref[...], preferred_element_type=F32)

    @pl.when(i >= steps + q_tiles)
    def _():
        out_ref[...] = jnp.dot(normed_ref[...], wkv_ref[...], preferred_element_type=F32)


def qkv_proj(x_rows, gain, w_query, w_kv, first_row, rows, deps):
    width = x_rows.shape[1]
    steps = rows // NORM_ROWS
    q_tiles = w_query.shape[1] // TILE
    kv_tiles = w_kv.shape[1] // TILE
    cols = w_query.shape[1] + w_kv.shape[1]
    return pl.pallas_call(
        functools.partial(qkv_kernel, steps, q_tiles),
        grid=(steps + q_tiles + kv_tiles,),
        in_specs=[
            pl.BlockSpec((NORM_ROWS, width), lambda i: (first_row // NORM_ROWS + jnp.minimum(i, steps - 1), 0)),
            pl.BlockSpec((1, width), lambda i: (0, 0)),
            pl.BlockSpec((width, TILE), lambda i: (0, jnp.clip(i - steps, 0, q_tiles - 1))),
            pl.BlockSpec((width, TILE), lambda i: (0, jnp.clip(i - steps - q_tiles, 0, kv_tiles - 1))),
        ] + [ANY] * len(deps),
        out_specs=pl.BlockSpec((rows, TILE), lambda i: (0, jnp.maximum(i - steps, 0))),
        out_shape=jax.ShapeDtypeStruct((rows, cols), F32),
        scratch_shapes=[pltpu.VMEM((rows, width), BF16)],
        compiler_params=pltpu.CompilerParams(vmem_limit_bytes=50 * 2**20),
        cost_estimate=pl.CostEstimate(flops=2 * rows * width * cols, bytes_accessed=width * cols * 2 + rows * width * 2 + rows * cols * 4, transcendentals=0),
        name="qkv_proj",
    )(x_rows, gain, w_query, w_kv, *deps)


def gated_kernel(steps, h_ref, gain_ref, gate_ref, up_ref, *rest):
    out_ref, normed_ref = rest[-2:]
    i = pl.program_id(0)

    @pl.when(i < steps)
    def _():
        norm_into([h_ref.at[part] for part in range(h_ref.shape[0])], gain_ref, normed_ref, pl.multiple_of(i * NORM_ROWS, NORM_ROWS))

    @pl.when(i >= steps)
    def _():
        gate = jnp.dot(normed_ref[...], gate_ref[...], preferred_element_type=F32)
        up = jnp.dot(normed_ref[...], up_ref[...], preferred_element_type=F32)
        out_ref[...] = (jax.nn.silu(gate) * up).astype(BF16)


def gated_proj(hidden, gain, w_gate, w_up, deps):
    parts, rows, part_cols = hidden.shape
    width, cols = w_gate.shape
    steps = rows // NORM_ROWS
    weight = pl.BlockSpec((width, TILE), lambda i: (0, jnp.maximum(i - steps, 0)))
    return pl.pallas_call(
        functools.partial(gated_kernel, steps),
        grid=(steps + cols // TILE,),
        in_specs=[
            pl.BlockSpec((parts, NORM_ROWS, part_cols), lambda i: (0, jnp.minimum(i, steps - 1), 0)),
            pl.BlockSpec((1, width), lambda i: (0, 0)),
            weight,
            weight,
        ] + [ANY] * len(deps),
        out_specs=pl.BlockSpec((rows, TILE), lambda i: (0, jnp.maximum(i - steps, 0))),
        out_shape=jax.ShapeDtypeStruct((rows, cols), BF16),
        scratch_shapes=[pltpu.VMEM((rows, width), BF16)],
        compiler_params=pltpu.CompilerParams(vmem_limit_bytes=50 * 2**20),
        cost_estimate=pl.CostEstimate(flops=4 * rows * width * cols, bytes_accessed=width * cols * 4 + rows * width * 2 + rows * cols * 2, transcendentals=rows * cols),
        name="gated_proj",
    )(hidden, gain, w_gate, w_up, *deps)


def out_proj_kernel(n_far, place_ref, heads_ref, x_ref, own_ref, near_ref, *rest):
    far_refs = rest[:n_far]
    h_ref, token_ref = rest[-2:]
    token_ref[...] = jnp.zeros_like(token_ref)
    tp_index, dp_index = place_ref[0], place_ref[1]
    total = x_ref[...].astype(F32)
    half = far_refs[0].shape[0]
    for hop, block in enumerate((own_ref, near_ref)):
        total = total + jnp.dot(heads_ref[tp_index ^ hop], block[...], preferred_element_type=F32).astype(BF16).astype(F32)
    for hop in range(2, 2 + len(far_refs) // 2):
        part = 0.0
        for side in range(2):
            start = pl.multiple_of((dp_index ^ side) * half, half)
            part = part + jnp.dot(heads_ref[tp_index ^ hop, :, pl.ds(start, half)], far_refs[2 * (hop - 2) + side][...], preferred_element_type=F32)
        total = total + part.astype(BF16).astype(F32)
    h_ref[...] = total.astype(BF16)


def out_proj(place, heads, x_rows, w_out, near, far, first_row, deps):
    parts, rows, width = heads.shape
    cols = near.shape[1]
    block = 256
    steps = cols // block
    half = far[0].shape[0]
    return pl.pallas_call(
        functools.partial(out_proj_kernel, len(far)),
        grid_spec=pltpu.PrefetchScalarGridSpec(
            num_scalar_prefetch=1,
            grid=(steps,),
            in_specs=[
                pl.BlockSpec((parts, rows, width), lambda n, place: (0, 0, 0)),
                pl.BlockSpec((rows, block), lambda n, place: (first_row // rows, place[0] * steps + n)) if first_row % rows == 0 else pl.BlockSpec((pl.Element(rows), pl.Element(block)), lambda n, place: (first_row, (place[0] * steps + n) * block)),
                pl.BlockSpec((width, block), lambda n, place: (0, place[0] * steps + n)),
                pl.BlockSpec((width, block), lambda n, place: (0, n)),
            ] + [pl.BlockSpec((half, block), lambda n, place: (0, n))] * len(far) + [ANY] * len(deps),
            out_specs=[pl.BlockSpec((rows, block), lambda n, place: (0, n)), pl.BlockSpec((8, 128), lambda n, place: (0, 0))],
        ),
        out_shape=[jax.ShapeDtypeStruct((rows, cols), BF16), jax.ShapeDtypeStruct((8, 128), F32)],
        compiler_params=pltpu.CompilerParams(vmem_limit_bytes=56 * 2**20),
        cost_estimate=pl.CostEstimate(flops=2 * parts * rows * width * cols, bytes_accessed=parts * (rows + cols) * width * 2, transcendentals=0),
        name="out_proj",
    )(place, heads, x_rows, w_out, near, *far, *deps)


def sum_kernel(place_ref, received_ref, h_ref, *rest):
    out_ref = rest[-1]
    parts, _, cols = h_ref.shape
    for part in range(parts):
        span = slice(part * cols, (part + 1) * cols)
        total = received_ref[0, :, span].astype(F32)
        for source in range(1, parts):
            total = total + received_ref[source, :, span].astype(F32)
        out_ref[:, span] = (h_ref[part].astype(F32) + total).astype(BF16)


def sum_rows(place, received, hidden, deps):
    parts, rows, width = received.shape
    cols = hidden.shape[2]
    block = 48
    steps = rows // block
    return pl.pallas_call(
        sum_kernel,
        grid_spec=pltpu.PrefetchScalarGridSpec(
            num_scalar_prefetch=1,
            grid=(steps,),
            in_specs=[
                pl.BlockSpec((parts, block, width), lambda i, place: (0, i, 0)),
                pl.BlockSpec((parts, block, cols), lambda i, place: (0, place[0] * steps + i, 0)),
            ] + [ANY] * len(deps),
            out_specs=pl.BlockSpec((block, width), lambda i, place: (i, 0)),
        ),
        out_shape=jax.ShapeDtypeStruct((rows, width), BF16),
        cost_estimate=pl.CostEstimate(flops=rows * width * 600, bytes_accessed=rows * width * 12, transcendentals=0),
        name="sum_rows",
    )(place, received, hidden, *deps)


def store_kernel(*refs):
    refs[-1][...] = refs[0][...]


def store_rows(y, y_part, first_row, total_rows, deps):
    rows, width = y_part.shape
    block = 128
    return pl.pallas_call(
        store_kernel,
        grid=(rows // block,),
        in_specs=[pl.BlockSpec((block, width), lambda i: (i, 0))] + [ANY] * (len(deps) + (y is not None)),
        out_specs=pl.BlockSpec((block, width), lambda i: (first_row // block + i, 0)),
        out_shape=jax.ShapeDtypeStruct((total_rows, width), BF16),
        input_output_aliases={} if y is None else {1: 0},
        cost_estimate=pl.CostEstimate(flops=rows * width * 300, bytes_accessed=rows * width * 4, transcendentals=0),
        name="store_rows",
    )(*([y_part] if y is None else [y_part, y]), *deps)


def solution(mesh):
    tp_size = mesh.shape["tp"]
    dp_size = mesh.shape["dp"]

    def layer_shard(x, seq_lens, w_query, w_key, w_value, w_out, w_gate, w_up, w_down, attn_gain, mlp_gain, k_cache, v_cache):
        batch_size, seq_len, width = x.shape
        kv_local, head_dim = k_cache.shape[2:]
        q_width = w_query.shape[1]
        tp_index = lax.axis_index("tp")
        dp_index = lax.axis_index("dp")
        place = jnp.stack([tp_index, dp_index]).astype(jnp.int32)
        part_cols = width // tp_size
        total_rows = batch_size * seq_len
        x_rows = x.reshape(total_rows, width)
        chunks = len(CHUNKS)
        first = [sum(CHUNKS[:c]) for c in range(chunks)]

        half = q_width // dp_size
        swaps = [[(i, i ^ hop) for i in range(tp_size)] for hop in range(tp_size)]
        dp_ring = [(i, (i + 1) % dp_size) for i in range(dp_size)]
        mine = []
        other = []
        for hop in range(2, tp_size):
            block = lax.dynamic_slice(w_out, (dp_index * half, (tp_index ^ hop) * part_cols), (half, part_cols))
            mine.append(lax.ppermute(block, "tp", swaps[hop]))
            other.append(lax.ppermute(mine[-1], "dp", dp_ring))
        block = lax.dynamic_slice_in_dim(w_out, (tp_index ^ 1) * part_cols, part_cols, axis=1)
        near = lax.ppermute(block, "tp", swaps[1])

        w_kv = jnp.concatenate([w_key, w_value], axis=1)
        cos_tab, sin_tab = rope_tables(seq_len, head_dim)
        gain = attn_gain.astype(F32).reshape(1, width)
        mlp_gain32 = mlp_gain.astype(F32).reshape(1, width)

        heads = []
        new_keys = []
        new_values = []
        deps = []
        for c in range(chunks):
            rows = CHUNKS[c] * seq_len
            if c == 2:
                deps = deps + [mine[0]]
            qkv = qkv_proj(x_rows, gain, w_query, w_kv, first[c] * seq_len, rows, deps)
            out, keys, values = attention(seq_lens, qkv, cos_tab, sin_tab, first[c], CHUNKS[c], seq_len, head_dim, kv_local, mine[1:] if c == 2 else [])
            deps = [keys]
            heads.append(lax.all_gather(out, "tp", axis=0))
            new_keys.append(keys)
            new_values.append(values)

        hidden = {}
        received = {}
        gathered = {}
        y = None

        def project(c, deps):
            local, token = out_proj(place, heads[c], x_rows, w_out, near, [mine[0], other[0], mine[1], other[1]], first[c] * seq_len, deps)
            hidden[c] = lax.all_gather(local, "tp", axis=0)
            return [token]

        def finish(c, deps):
            y_rows = sum_rows(place, received[c], hidden[c], deps)
            gathered[c] = lax.all_gather(y_rows, "tp", axis=0, tiled=True)
            return [y_rows]

        def store(c, y, deps):
            return store_rows(y, gathered[c], first[c] * seq_len, total_rows, deps)

        deps = project(0, deps)
        deps = project(1, deps)
        for c in range(chunks):
            rows = CHUNKS[c] * seq_len
            gated = gated_proj(hidden[c], mlp_gain32, w_gate, w_up, deps)
            part = jnp.dot(gated, w_down, preferred_element_type=F32).astype(BF16)
            received[c] = lax.all_to_all(part.reshape(tp_size, rows // tp_size, width), "tp", 0, 0, tiled=True)
            deps = [part]
            if c >= 1:
                deps = finish(c - 1, deps)
            if c >= 3:
                y = store(c - 3, y, deps)
                deps = [y]
            if c + 2 < chunks:
                deps = project(c + 2, deps)
        y = store(chunks - 3, y, [])
        y = store(chunks - 2, y, [])
        finish(chunks - 1, [])
        y = store(chunks - 1, y, [])

        def cache(old, new):
            new = jnp.concatenate(new, axis=0).reshape(batch_size, seq_len, kv_local, head_dim)
            return jnp.concatenate([new, old[:, seq_len:]], axis=1)

        return y.reshape(x.shape), cache(k_cache, new_keys), cache(v_cache, new_values)

    cache_spec = P("dp", None, "tp", None)
    return jax.shard_map(layer_shard, mesh=mesh, in_specs=(P("dp", None, None), P("dp"), P(None, "tp"), P(None, "tp"), P(None, "tp"), P("tp", None), P(None, "tp"), P(None, "tp"), P("tp", None), P(), P(), cache_spec, cache_spec), out_specs=(P("dp", None, None), cache_spec, cache_spec), check_vma=False)
```

```python
import functools

import jax
import jax.numpy as jnp
from jax import lax
from jax.experimental import pallas as pl
from jax.experimental.pallas import tpu as pltpu
from jax.sharding import PartitionSpec as P


EPS = 1e-5
ROPE_BASE = 10000.0
CHUNKS = (1, 2, 2, 2, 1)
F32 = jnp.float32
BF16 = jnp.bfloat16
ANY = pl.BlockSpec(memory_space=pltpu.MemorySpace.HBM)


def rope_tables(seq_len, head_dim):
    inv_freq = ROPE_BASE ** (-jnp.arange(0, head_dim, 2).astype(F32) / head_dim)
    angles = jnp.arange(seq_len).astype(F32)[:, None] * inv_freq[None, :]
    cos_tab = jnp.repeat(jnp.cos(angles), 2, axis=1)
    sin_tab = jnp.sin(angles)
    sin_tab = jnp.stack([-sin_tab, sin_tab], axis=-1).reshape(seq_len, head_dim)
    return cos_tab, sin_tab


def turn(vecs, cos_tab, sin_tab, even_lane):
    width = vecs.shape[1]
    swapped = jnp.where(even_lane, pltpu.roll(vecs, width - 1, 1), pltpu.roll(vecs, 1, 1))
    return vecs * cos_tab + swapped * sin_tab


def attention_kernel(first_seq, group_size, head_dim, lens_ref, q_ref, k_ref, v_ref, cos_ref, sin_ref, *rest):
    o_ref, k_out_ref, v_out_ref = rest[-3:]
    seq_len = q_ref.shape[0]
    length = lens_ref[first_seq + pl.program_id(0)]
    cos_tab = cos_ref[...]
    sin_tab = sin_ref[...]
    even_lane = lax.broadcasted_iota(jnp.int32, (seq_len, head_dim), 1) % 2 == 0
    valid = lax.broadcasted_iota(jnp.int32, (seq_len, head_dim), 0) < length
    keys = jnp.where(valid, turn(k_ref[...], cos_tab, sin_tab, even_lane), 0.0).astype(BF16)
    values = jnp.where(valid, v_ref[...], 0.0).astype(BF16)
    k_out_ref[...] = keys
    v_out_ref[...] = values
    step = 128
    turned = []
    for head in range(group_size):
        cols = slice(head * head_dim, (head + 1) * head_dim)
        turned.append(turn(q_ref[:, cols], cos_tab, sin_tab, even_lane).astype(BF16))
    factor = head_dim ** -0.5 * 1.4426950408889634
    for start in range(0, seq_len, step):
        stop = start + step
        queries = jnp.concatenate([head[start:stop] for head in turned], axis=0)
        scores = lax.dot_general(queries, keys[:stop], (((1,), (1,)), ((), ())), preferred_element_type=F32)
        row = lax.broadcasted_iota(jnp.int32, (step, stop), 0) + start
        col = lax.broadcasted_iota(jnp.int32, (step, stop), 1)
        hide = jnp.where((col <= row) & (col < length), 0.0, -jnp.inf)
        scores = scores.reshape(group_size, step, stop) + hide[None]
        exps = jnp.exp2((scores - jnp.max(scores, axis=2, keepdims=True)) * factor)
        probs = (exps * (1.0 / jnp.sum(exps, axis=2, keepdims=True))).astype(BF16)
        mixed = jnp.dot(probs.reshape(group_size * step, stop), values[:stop], preferred_element_type=F32).astype(BF16)
        for head in range(group_size):
            o_ref[start:stop, head * head_dim:(head + 1) * head_dim] = mixed[head * step:(head + 1) * step]


def attention(lens, qkv, cos_tab, sin_tab, first_seq, n_seq, seq_len, head_dim, kv_local, deps):
    rows = n_seq * seq_len
    heads = qkv.shape[1] // head_dim - 2 * kv_local
    group_size = heads // kv_local
    wide = group_size * head_dim
    per_head = [pl.BlockSpec((seq_len, head_dim), functools.partial(lambda offset, b, g, lens: (b, offset + g), offset)) for offset in (heads, heads + kv_local, 0)]
    grouped = pl.BlockSpec((seq_len, wide), lambda b, g, lens: (b, g))
    table = pl.BlockSpec((seq_len, head_dim), lambda b, g, lens: (0, 0))
    return pl.pallas_call(
        functools.partial(attention_kernel, first_seq, group_size, head_dim),
        grid_spec=pltpu.PrefetchScalarGridSpec(
            num_scalar_prefetch=1,
            grid=(n_seq, kv_local),
            in_specs=[grouped, per_head[0], per_head[1], table, table] + [ANY] * len(deps),
            out_specs=[grouped, per_head[2], per_head[2]],
        ),
        out_shape=[
            jax.ShapeDtypeStruct((rows, heads * head_dim), BF16),
            jax.ShapeDtypeStruct((rows, kv_local * head_dim), BF16),
            jax.ShapeDtypeStruct((rows, kv_local * head_dim), BF16),
        ],
        cost_estimate=pl.CostEstimate(flops=16 * rows * heads * head_dim * seq_len, bytes_accessed=rows * heads * head_dim * 8, transcendentals=rows * seq_len * heads),
        name="attention",
    )(lens, qkv, qkv, qkv, cos_tab, sin_tab, *deps)


NORM_ROWS = 128
NORM_COLS = 512
TILE = 256


def inv_rms_of(parts):
    total = 0.0
    width = 0
    for part in parts:
        for start in range(0, part.shape[1], NORM_COLS // 2):
            x32 = part[:, start:start + NORM_COLS // 2].astype(F32)
            square = x32 * x32
            for lane in range(0, square.shape[1], 128):
                total = total + square[:, lane:lane + 128]
        width += part.shape[1]
    return lax.rsqrt(jnp.sum(total, axis=1, keepdims=True) / width + EPS)


def norm_into(parts, gain_ref, normed_ref, row):
    inv_rms = inv_rms_of(parts)
    column = 0
    for part in parts:
        for start in range(0, part.shape[1], NORM_COLS // 2):
            span = slice(column, column + NORM_COLS // 2)
            normed_ref[pl.ds(row, part.shape[0]), span] = (part[:, start:start + NORM_COLS // 2].astype(F32) * inv_rms * gain_ref[:, span]).astype(BF16)
            column += NORM_COLS // 2


def qkv_kernel(steps, q_tiles, x_ref, gain_ref, wq_ref, wkv_ref, *rest):
    out_ref, normed_ref = rest[-2:]
    i = pl.program_id(0)

    @pl.when(i < steps)
    def _():
        norm_into([x_ref], gain_ref, normed_ref, pl.multiple_of(i * NORM_ROWS, NORM_ROWS))

    @pl.when((i >= steps) & (i < steps + q_tiles))
    def _():
        out_ref[...] = jnp.dot(normed_ref[...], wq_ref[...], preferred_element_type=F32)

    @pl.when(i >= steps + q_tiles)
    def _():
        out_ref[...] = jnp.dot(normed_ref[...], wkv_ref[...], preferred_element_type=F32)


def qkv_proj(x_rows, gain, w_query, w_kv, first_row, rows, deps):
    width = x_rows.shape[1]
    steps = rows // NORM_ROWS
    q_tiles = w_query.shape[1] // TILE
    kv_tiles = w_kv.shape[1] // TILE
    cols = w_query.shape[1] + w_kv.shape[1]
    return pl.pallas_call(
        functools.partial(qkv_kernel, steps, q_tiles),
        grid=(steps + q_tiles + kv_tiles,),
        in_specs=[
            pl.BlockSpec((NORM_ROWS, width), lambda i: (first_row // NORM_ROWS + jnp.minimum(i, steps - 1), 0)),
            pl.BlockSpec((1, width), lambda i: (0, 0)),
            pl.BlockSpec((width, TILE), lambda i: (0, jnp.clip(i - steps, 0, q_tiles - 1))),
            pl.BlockSpec((width, TILE), lambda i: (0, jnp.clip(i - steps - q_tiles, 0, kv_tiles - 1))),
        ] + [ANY] * len(deps),
        out_specs=pl.BlockSpec((rows, TILE), lambda i: (0, jnp.maximum(i - steps, 0))),
        out_shape=jax.ShapeDtypeStruct((rows, cols), F32),
        scratch_shapes=[pltpu.VMEM((rows, width), BF16)],
        compiler_params=pltpu.CompilerParams(vmem_limit_bytes=50 * 2**20),
        cost_estimate=pl.CostEstimate(flops=2 * rows * width * cols, bytes_accessed=width * cols * 2 + rows * width * 2 + rows * cols * 4, transcendentals=0),
        name="qkv_proj",
    )(x_rows, gain, w_query, w_kv, *deps)


def gated_kernel(steps, h_ref, gain_ref, gate_ref, up_ref, *rest):
    out_ref, normed_ref = rest[-2:]
    i = pl.program_id(0)

    @pl.when(i < steps)
    def _():
        norm_into([h_ref.at[part] for part in range(h_ref.shape[0])], gain_ref, normed_ref, pl.multiple_of(i * NORM_ROWS, NORM_ROWS))

    @pl.when(i >= steps)
    def _():
        gate = jnp.dot(normed_ref[...], gate_ref[...], preferred_element_type=F32)
        up = jnp.dot(normed_ref[...], up_ref[...], preferred_element_type=F32)
        out_ref[...] = (jax.nn.silu(gate) * up).astype(BF16)


def gated_proj(hidden, gain, w_gate, w_up, deps):
    parts, rows, part_cols = hidden.shape
    width, cols = w_gate.shape
    steps = rows // NORM_ROWS
    weight = pl.BlockSpec((width, TILE), lambda i: (0, jnp.maximum(i - steps, 0)))
    return pl.pallas_call(
        functools.partial(gated_kernel, steps),
        grid=(steps + cols // TILE,),
        in_specs=[
            pl.BlockSpec((parts, NORM_ROWS, part_cols), lambda i: (0, jnp.minimum(i, steps - 1), 0)),
            pl.BlockSpec((1, width), lambda i: (0, 0)),
            weight,
            weight,
        ] + [ANY] * len(deps),
        out_specs=pl.BlockSpec((rows, TILE), lambda i: (0, jnp.maximum(i - steps, 0))),
        out_shape=jax.ShapeDtypeStruct((rows, cols), BF16),
        scratch_shapes=[pltpu.VMEM((rows, width), BF16)],
        compiler_params=pltpu.CompilerParams(vmem_limit_bytes=50 * 2**20),
        cost_estimate=pl.CostEstimate(flops=4 * rows * width * cols, bytes_accessed=width * cols * 4 + rows * width * 2 + rows * cols * 2, transcendentals=rows * cols),
        name="gated_proj",
    )(hidden, gain, w_gate, w_up, *deps)


def out_proj_kernel(n_far, place_ref, heads_ref, x_ref, own_ref, near_ref, *rest):
    far_refs = rest[:n_far]
    h_ref, token_ref = rest[-2:]
    token_ref[...] = jnp.zeros_like(token_ref)
    tp_index, dp_index = place_ref[0], place_ref[1]
    total = x_ref[...].astype(F32)
    half = far_refs[0].shape[0]
    for hop, block in enumerate((own_ref, near_ref)):
        total = total + jnp.dot(heads_ref[tp_index ^ hop], block[...], preferred_element_type=F32).astype(BF16).astype(F32)
    for hop in range(2, 2 + len(far_refs) // 2):
        part = 0.0
        for side in range(2):
            start = pl.multiple_of((dp_index ^ side) * half, half)
            part = part + jnp.dot(heads_ref[tp_index ^ hop, :, pl.ds(start, half)], far_refs[2 * (hop - 2) + side][...], preferred_element_type=F32)
        total = total + part.astype(BF16).astype(F32)
    h_ref[...] = total.astype(BF16)


def out_proj(place, heads, x_rows, w_out, near, far, first_row, deps):
    parts, rows, width = heads.shape
    cols = near.shape[1]
    block = 256
    steps = cols // block
    half = far[0].shape[0]
    return pl.pallas_call(
        functools.partial(out_proj_kernel, len(far)),
        grid_spec=pltpu.PrefetchScalarGridSpec(
            num_scalar_prefetch=1,
            grid=(steps,),
            in_specs=[
                pl.BlockSpec((parts, rows, width), lambda n, place: (0, 0, 0)),
                pl.BlockSpec((rows, block), lambda n, place: (first_row // rows, place[0] * steps + n)) if first_row % rows == 0 else pl.BlockSpec((pl.Element(rows), pl.Element(block)), lambda n, place: (first_row, (place[0] * steps + n) * block)),
                pl.BlockSpec((width, block), lambda n, place: (0, place[0] * steps + n)),
                pl.BlockSpec((width, block), lambda n, place: (0, n)),
            ] + [pl.BlockSpec((half, block), lambda n, place: (0, n))] * len(far) + [ANY] * len(deps),
            out_specs=[pl.BlockSpec((rows, block), lambda n, place: (0, n)), pl.BlockSpec((8, 128), lambda n, place: (0, 0))],
        ),
        out_shape=[jax.ShapeDtypeStruct((rows, cols), BF16), jax.ShapeDtypeStruct((8, 128), F32)],
        compiler_params=pltpu.CompilerParams(vmem_limit_bytes=56 * 2**20),
        cost_estimate=pl.CostEstimate(flops=2 * parts * rows * width * cols, bytes_accessed=parts * (rows + cols) * width * 2, transcendentals=0),
        name="out_proj",
    )(place, heads, x_rows, w_out, near, *far, *deps)


def sum_kernel(place_ref, received_ref, h_ref, *rest):
    out_ref = rest[-1]
    parts, _, cols = h_ref.shape
    for part in range(parts):
        span = slice(part * cols, (part + 1) * cols)
        total = received_ref[0, :, span].astype(F32)
        for source in range(1, parts):
            total = total + received_ref[source, :, span].astype(F32)
        out_ref[:, span] = (h_ref[part].astype(F32) + total).astype(BF16)


def sum_rows(place, received, hidden, deps):
    parts, rows, width = received.shape
    cols = hidden.shape[2]
    block = 48
    steps = rows // block
    return pl.pallas_call(
        sum_kernel,
        grid_spec=pltpu.PrefetchScalarGridSpec(
            num_scalar_prefetch=1,
            grid=(steps,),
            in_specs=[
                pl.BlockSpec((parts, block, width), lambda i, place: (0, i, 0)),
                pl.BlockSpec((parts, block, cols), lambda i, place: (0, place[0] * steps + i, 0)),
            ] + [ANY] * len(deps),
            out_specs=pl.BlockSpec((block, width), lambda i, place: (i, 0)),
        ),
        out_shape=jax.ShapeDtypeStruct((rows, width), BF16),
        cost_estimate=pl.CostEstimate(flops=rows * width * 600, bytes_accessed=rows * width * 12, transcendentals=0),
        name="sum_rows",
    )(place, received, hidden, *deps)


def store_kernel(*refs):
    refs[-1][...] = refs[0][...]


def store_rows(y, y_part, first_row, total_rows, deps):
    rows, width = y_part.shape
    block = 128
    return pl.pallas_call(
        store_kernel,
        grid=(rows // block,),
        in_specs=[pl.BlockSpec((block, width), lambda i: (i, 0))] + [ANY] * (len(deps) + (y is not None)),
        out_specs=pl.BlockSpec((block, width), lambda i: (first_row // block + i, 0)),
        out_shape=jax.ShapeDtypeStruct((total_rows, width), BF16),
        input_output_aliases={} if y is None else {1: 0},
        cost_estimate=pl.CostEstimate(flops=rows * width * 300, bytes_accessed=rows * width * 4, transcendentals=0),
        name="store_rows",
    )(*([y_part] if y is None else [y_part, y]), *deps)


def solution(mesh):
    tp_size = mesh.shape["tp"]
    dp_size = mesh.shape["dp"]

    def layer_shard(x, seq_lens, w_query, w_key, w_value, w_out, w_gate, w_up, w_down, attn_gain, mlp_gain, k_cache, v_cache):
        batch_size, seq_len, width = x.shape
        kv_local, head_dim = k_cache.shape[2:]
        q_width = w_query.shape[1]
        tp_index = lax.axis_index("tp")
        dp_index = lax.axis_index("dp")
        place = jnp.stack([tp_index, dp_index]).astype(jnp.int32)
        part_cols = width // tp_size
        total_rows = batch_size * seq_len
        x_rows = x.reshape(total_rows, width)
        chunks = len(CHUNKS)
        first = [sum(CHUNKS[:c]) for c in range(chunks)]

        half = q_width // dp_size
        swaps = [[(i, i ^ hop) for i in range(tp_size)] for hop in range(tp_size)]
        dp_ring = [(i, (i + 1) % dp_size) for i in range(dp_size)]
        mine = []
        other = []
        for hop in range(2, tp_size):
            block = lax.dynamic_slice(w_out, (dp_index * half, (tp_index ^ hop) * part_cols), (half, part_cols))
            mine.append(lax.ppermute(block, "tp", swaps[hop]))
            other.append(lax.ppermute(mine[-1], "dp", dp_ring))
        block = lax.dynamic_slice_in_dim(w_out, (tp_index ^ 1) * part_cols, part_cols, axis=1)
        near = lax.ppermute(block, "tp", swaps[1])

        w_kv = jnp.concatenate([w_key, w_value], axis=1)
        cos_tab, sin_tab = rope_tables(seq_len, head_dim)
        gain = attn_gain.astype(F32).reshape(1, width)
        mlp_gain32 = mlp_gain.astype(F32).reshape(1, width)

        heads = []
        new_keys = []
        new_values = []
        deps = []
        for c in range(chunks):
            rows = CHUNKS[c] * seq_len
            if c == 2:
                deps = deps + [mine[0]]
            qkv = qkv_proj(x_rows, gain, w_query, w_kv, first[c] * seq_len, rows, deps)
            out, keys, values = attention(seq_lens, qkv, cos_tab, sin_tab, first[c], CHUNKS[c], seq_len, head_dim, kv_local, mine[1:] if c == 2 else [])
            deps = [keys]
            heads.append(lax.all_gather(out, "tp", axis=0))
            new_keys.append(keys)
            new_values.append(values)

        hidden = {}
        received = {}
        gathered = {}
        y = None

        def project(c, deps):
            local, token = out_proj(place, heads[c], x_rows, w_out, near, [mine[0], other[0], mine[1], other[1]], first[c] * seq_len, deps)
            hidden[c] = lax.all_gather(local, "tp", axis=0)
            return [token]

        def finish(c, deps):
            y_rows = sum_rows(place, received[c], hidden[c], deps)
            gathered[c] = lax.all_gather(y_rows, "tp", axis=0, tiled=True)
            return [y_rows]

        def store(c, y, deps):
            return store_rows(y, gathered[c], first[c] * seq_len, total_rows, deps)

        deps = project(0, deps)
        deps = project(1, deps)
        for c in range(chunks):
            rows = CHUNKS[c] * seq_len
            gated = gated_proj(hidden[c], mlp_gain32, w_gate, w_up, deps)
            if c == 1:
                project(2, [gated])
            part = jnp.dot(gated, w_down, preferred_element_type=F32).astype(BF16)
            received[c] = lax.all_to_all(part.reshape(tp_size, rows // tp_size, width), "tp", 0, 0, tiled=True)
            deps = [part]
            if c >= 1:
                deps = finish(c - 1, deps)
            if c >= 3:
                y = store(c - 3, y, deps)
                deps = [y]
            if c >= 1 and c + 2 < chunks:
                deps = project(c + 2, deps)

        def cache(old, new):
            new = jnp.concatenate(new, axis=0).reshape(batch_size, seq_len, kv_local, head_dim)
            return jnp.concatenate([new, old[:, seq_len:]], axis=1)

        caches = [cache(k_cache, new_keys), cache(v_cache, new_values)]
        y = store(chunks - 3, y, [])
        finish(chunks - 1, [y] + caches)
        y = store(chunks - 2, y, [])
        y = store(chunks - 1, y, [])

        return y.reshape(x.shape), caches[0], caches[1]

    cache_spec = P("dp", None, "tp", None)
    return jax.shard_map(layer_shard, mesh=mesh, in_specs=(P("dp", None, None), P("dp"), P(None, "tp"), P(None, "tp"), P(None, "tp"), P("tp", None), P(None, "tp"), P(None, "tp"), P("tp", None), P(), P(), cache_spec, cache_spec), out_specs=(P("dp", None, None), cache_spec, cache_spec), check_vma=False)
```

```python
import functools

import jax
import jax.numpy as jnp
from jax import lax
from jax.experimental import pallas as pl
from jax.experimental.pallas import tpu as pltpu
from jax.sharding import PartitionSpec as P


EPS = 1e-5
ROPE_BASE = 10000.0
CHUNKS = (1, 2, 2, 2, 1)
F32 = jnp.float32
BF16 = jnp.bfloat16
ANY = pl.BlockSpec(memory_space=pltpu.MemorySpace.HBM)


def rope_tables(seq_len, head_dim):
    inv_freq = ROPE_BASE ** (-jnp.arange(0, head_dim, 2).astype(F32) / head_dim)
    angles = jnp.arange(seq_len).astype(F32)[:, None] * inv_freq[None, :]
    cos_tab = jnp.repeat(jnp.cos(angles), 2, axis=1)
    sin_tab = jnp.sin(angles)
    sin_tab = jnp.stack([-sin_tab, sin_tab], axis=-1).reshape(seq_len, head_dim)
    return cos_tab, sin_tab


def turn(vecs, cos_tab, sin_tab, even_lane):
    width = vecs.shape[1]
    swapped = jnp.where(even_lane, pltpu.roll(vecs, width - 1, 1), pltpu.roll(vecs, 1, 1))
    return vecs * cos_tab + swapped * sin_tab


def attention_kernel(first_seq, group_size, head_dim, lens_ref, q_ref, k_ref, v_ref, cos_ref, sin_ref, *rest):
    o_ref, k_out_ref, v_out_ref = rest[-3:]
    seq_len = q_ref.shape[0]
    length = lens_ref[first_seq + pl.program_id(0)]
    cos_tab = cos_ref[...]
    sin_tab = sin_ref[...]
    even_lane = lax.broadcasted_iota(jnp.int32, (seq_len, head_dim), 1) % 2 == 0
    valid = lax.broadcasted_iota(jnp.int32, (seq_len, head_dim), 0) < length
    keys = jnp.where(valid, turn(k_ref[...], cos_tab, sin_tab, even_lane), 0.0).astype(BF16)
    values = jnp.where(valid, v_ref[...], 0.0).astype(BF16)
    k_out_ref[...] = keys
    v_out_ref[...] = values
    step = 128
    turned = []
    for head in range(group_size):
        cols = slice(head * head_dim, (head + 1) * head_dim)
        turned.append(turn(q_ref[:, cols], cos_tab, sin_tab, even_lane).astype(BF16))
    factor = head_dim ** -0.5 * 1.4426950408889634
    for start in range(0, seq_len, step):
        stop = start + step
        queries = jnp.concatenate([head[start:stop] for head in turned], axis=0)
        scores = lax.dot_general(queries, keys[:stop], (((1,), (1,)), ((), ())), preferred_element_type=F32)
        row = lax.broadcasted_iota(jnp.int32, (step, stop), 0) + start
        col = lax.broadcasted_iota(jnp.int32, (step, stop), 1)
        hide = jnp.where((col <= row) & (col < length), 0.0, -jnp.inf)
        scores = scores.reshape(group_size, step, stop) + hide[None]
        exps = jnp.exp2((scores - jnp.max(scores, axis=2, keepdims=True)) * factor)
        probs = (exps * (1.0 / jnp.sum(exps, axis=2, keepdims=True))).astype(BF16)
        mixed = jnp.dot(probs.reshape(group_size * step, stop), values[:stop], preferred_element_type=F32).astype(BF16)
        for head in range(group_size):
            o_ref[start:stop, head * head_dim:(head + 1) * head_dim] = mixed[head * step:(head + 1) * step]


def attention(lens, qkv, cos_tab, sin_tab, first_seq, n_seq, seq_len, head_dim, kv_local, deps):
    rows = n_seq * seq_len
    heads = qkv.shape[1] // head_dim - 2 * kv_local
    group_size = heads // kv_local
    wide = group_size * head_dim
    per_head = [pl.BlockSpec((seq_len, head_dim), functools.partial(lambda offset, b, g, lens: (b, offset + g), offset)) for offset in (heads, heads + kv_local, 0)]
    grouped = pl.BlockSpec((seq_len, wide), lambda b, g, lens: (b, g))
    table = pl.BlockSpec((seq_len, head_dim), lambda b, g, lens: (0, 0))
    return pl.pallas_call(
        functools.partial(attention_kernel, first_seq, group_size, head_dim),
        grid_spec=pltpu.PrefetchScalarGridSpec(
            num_scalar_prefetch=1,
            grid=(n_seq, kv_local),
            in_specs=[grouped, per_head[0], per_head[1], table, table] + [ANY] * len(deps),
            out_specs=[grouped, per_head[2], per_head[2]],
        ),
        out_shape=[
            jax.ShapeDtypeStruct((rows, heads * head_dim), BF16),
            jax.ShapeDtypeStruct((rows, kv_local * head_dim), BF16),
            jax.ShapeDtypeStruct((rows, kv_local * head_dim), BF16),
        ],
        cost_estimate=pl.CostEstimate(flops=16 * rows * heads * head_dim * seq_len, bytes_accessed=rows * heads * head_dim * 8, transcendentals=rows * seq_len * heads),
        name="attention",
    )(lens, qkv, qkv, qkv, cos_tab, sin_tab, *deps)


NORM_ROWS = 128
NORM_COLS = 512
TILE = 256


def inv_rms_of(parts):
    total = 0.0
    width = 0
    for part in parts:
        for start in range(0, part.shape[1], NORM_COLS // 2):
            x32 = part[:, start:start + NORM_COLS // 2].astype(F32)
            square = x32 * x32
            for lane in range(0, square.shape[1], 128):
                total = total + square[:, lane:lane + 128]
        width += part.shape[1]
    return lax.rsqrt(jnp.sum(total, axis=1, keepdims=True) / width + EPS)


def norm_into(parts, gain_ref, normed_ref, row):
    inv_rms = inv_rms_of(parts)
    column = 0
    for part in parts:
        for start in range(0, part.shape[1], NORM_COLS // 2):
            span = slice(column, column + NORM_COLS // 2)
            normed_ref[pl.ds(row, part.shape[0]), span] = (part[:, start:start + NORM_COLS // 2].astype(F32) * inv_rms * gain_ref[:, span]).astype(BF16)
            column += NORM_COLS // 2


def qkv_kernel(steps, q_tiles, x_ref, gain_ref, wq_ref, wkv_ref, *rest):
    out_ref, normed_ref = rest[-2:]
    i = pl.program_id(0)

    @pl.when(i < steps)
    def _():
        norm_into([x_ref], gain_ref, normed_ref, pl.multiple_of(i * NORM_ROWS, NORM_ROWS))

    @pl.when((i >= steps) & (i < steps + q_tiles))
    def _():
        out_ref[...] = jnp.dot(normed_ref[...], wq_ref[...], preferred_element_type=F32)

    @pl.when(i >= steps + q_tiles)
    def _():
        out_ref[...] = jnp.dot(normed_ref[...], wkv_ref[...], preferred_element_type=F32)


def qkv_proj(x_rows, gain, w_query, w_kv, first_row, rows, deps):
    width = x_rows.shape[1]
    steps = rows // NORM_ROWS
    q_tiles = w_query.shape[1] // TILE
    kv_tiles = w_kv.shape[1] // TILE
    cols = w_query.shape[1] + w_kv.shape[1]
    return pl.pallas_call(
        functools.partial(qkv_kernel, steps, q_tiles),
        grid=(steps + q_tiles + kv_tiles,),
        in_specs=[
            pl.BlockSpec((NORM_ROWS, width), lambda i: (first_row // NORM_ROWS + jnp.minimum(i, steps - 1), 0)),
            pl.BlockSpec((1, width), lambda i: (0, 0)),
            pl.BlockSpec((width, TILE), lambda i: (0, jnp.clip(i - steps, 0, q_tiles - 1))),
            pl.BlockSpec((width, TILE), lambda i: (0, jnp.clip(i - steps - q_tiles, 0, kv_tiles - 1))),
        ] + [ANY] * len(deps),
        out_specs=pl.BlockSpec((rows, TILE), lambda i: (0, jnp.maximum(i - steps, 0))),
        out_shape=jax.ShapeDtypeStruct((rows, cols), F32),
        scratch_shapes=[pltpu.VMEM((rows, width), BF16)],
        compiler_params=pltpu.CompilerParams(vmem_limit_bytes=50 * 2**20),
        cost_estimate=pl.CostEstimate(flops=2 * rows * width * cols, bytes_accessed=width * cols * 2 + rows * width * 2 + rows * cols * 4, transcendentals=0),
        name="qkv_proj",
    )(x_rows, gain, w_query, w_kv, *deps)


def gated_kernel(steps, h_ref, gain_ref, gate_ref, up_ref, *rest):
    out_ref, normed_ref = rest[-2:]
    i = pl.program_id(0)

    @pl.when(i < steps)
    def _():
        norm_into([h_ref.at[part] for part in range(h_ref.shape[0])], gain_ref, normed_ref, pl.multiple_of(i * NORM_ROWS, NORM_ROWS))

    @pl.when(i >= steps)
    def _():
        gate = jnp.dot(normed_ref[...], gate_ref[...], preferred_element_type=F32)
        up = jnp.dot(normed_ref[...], up_ref[...], preferred_element_type=F32)
        out_ref[...] = (jax.nn.silu(gate) * up).astype(BF16)


def gated_proj(hidden, gain, w_gate, w_up, deps):
    parts, rows, part_cols = hidden.shape
    width, cols = w_gate.shape
    steps = rows // NORM_ROWS
    weight = pl.BlockSpec((width, TILE), lambda i: (0, jnp.maximum(i - steps, 0)))
    return pl.pallas_call(
        functools.partial(gated_kernel, steps),
        grid=(steps + cols // TILE,),
        in_specs=[
            pl.BlockSpec((parts, NORM_ROWS, part_cols), lambda i: (0, jnp.minimum(i, steps - 1), 0)),
            pl.BlockSpec((1, width), lambda i: (0, 0)),
            weight,
            weight,
        ] + [ANY] * len(deps),
        out_specs=pl.BlockSpec((rows, TILE), lambda i: (0, jnp.maximum(i - steps, 0))),
        out_shape=jax.ShapeDtypeStruct((rows, cols), BF16),
        scratch_shapes=[pltpu.VMEM((rows, width), BF16)],
        compiler_params=pltpu.CompilerParams(vmem_limit_bytes=50 * 2**20),
        cost_estimate=pl.CostEstimate(flops=4 * rows * width * cols, bytes_accessed=width * cols * 4 + rows * width * 2 + rows * cols * 2, transcendentals=rows * cols),
        name="gated_proj",
    )(hidden, gain, w_gate, w_up, *deps)


def out_proj_kernel(n_far, place_ref, all_heads_ref, x_ref, own_ref, near_ref, *rest):
    far_refs = rest[:n_far]
    h_ref, token_ref, heads_ref, sems = rest[-4:]
    tp_index, dp_index = place_ref[0], place_ref[1]
    half = far_refs[0].shape[0]
    parts = heads_ref.shape[0]
    token_ref[...] = jnp.zeros_like(token_ref)
    copies = [pltpu.make_async_copy(all_heads_ref.at[tp_index ^ hop], heads_ref.at[hop], sems.at[hop]) for hop in range(parts)]

    def body(arriving):
        total = x_ref[...].astype(F32)
        for hop in range(parts):
            if arriving:
                copies[hop].wait()
            if hop < 2:
                part = jnp.dot(heads_ref[hop], (own_ref, near_ref)[hop][...], preferred_element_type=F32)
            else:
                part = 0.0
                for side in range(2):
                    start = pl.multiple_of((dp_index ^ side) * half, half)
                    part = part + jnp.dot(heads_ref[hop, :, pl.ds(start, half)], far_refs[2 * (hop - 2) + side][...], preferred_element_type=F32)
            total = total + part.astype(BF16).astype(F32)
        h_ref[...] = total.astype(BF16)

    @pl.when(pl.program_id(0) == 0)
    def _():
        for copy in copies:
            copy.start()
        body(True)

    @pl.when(pl.program_id(0) > 0)
    def _():
        body(False)


def out_proj(place, heads, x_rows, w_out, near, far, first_row, deps):
    parts, rows, width = heads.shape
    cols = near.shape[1]
    block = 256
    steps = cols // block
    half = far[0].shape[0]
    return pl.pallas_call(
        functools.partial(out_proj_kernel, len(far)),
        grid_spec=pltpu.PrefetchScalarGridSpec(
            num_scalar_prefetch=1,
            grid=(steps,),
            in_specs=[
                ANY,
                pl.BlockSpec((rows, block), lambda n, place: (first_row // rows, place[0] * steps + n)) if first_row % rows == 0 else pl.BlockSpec((pl.Element(rows), pl.Element(block)), lambda n, place: (first_row, (place[0] * steps + n) * block)),
                pl.BlockSpec((width, block), lambda n, place: (0, place[0] * steps + n)),
                pl.BlockSpec((width, block), lambda n, place: (0, n)),
            ] + [pl.BlockSpec((half, block), lambda n, place: (0, n))] * len(far) + [ANY] * len(deps),
            out_specs=[pl.BlockSpec((rows, block), lambda n, place: (0, n)), pl.BlockSpec((8, 128), lambda n, place: (0, 0))],
            scratch_shapes=[pltpu.VMEM((parts, rows, width), BF16), pltpu.SemaphoreType.DMA((parts,))],
        ),
        out_shape=[jax.ShapeDtypeStruct((rows, cols), BF16), jax.ShapeDtypeStruct((8, 128), F32)],
        compiler_params=pltpu.CompilerParams(vmem_limit_bytes=56 * 2**20),
        cost_estimate=pl.CostEstimate(flops=2 * parts * rows * width * cols, bytes_accessed=parts * (rows + cols) * width * 2, transcendentals=0),
        name="out_proj",
    )(place, heads, x_rows, w_out, near, *far, *deps)


def sum_kernel(place_ref, received_ref, h_ref, *rest):
    out_ref = rest[-1]
    parts, _, cols = h_ref.shape
    for part in range(parts):
        span = slice(part * cols, (part + 1) * cols)
        total = received_ref[0, :, span].astype(F32)
        for source in range(1, parts):
            total = total + received_ref[source, :, span].astype(F32)
        out_ref[:, span] = (h_ref[part].astype(F32) + total).astype(BF16)


def sum_rows(place, received, hidden, deps):
    parts, rows, width = received.shape
    cols = hidden.shape[2]
    block = 48
    steps = rows // block
    return pl.pallas_call(
        sum_kernel,
        grid_spec=pltpu.PrefetchScalarGridSpec(
            num_scalar_prefetch=1,
            grid=(steps,),
            in_specs=[
                pl.BlockSpec((parts, block, width), lambda i, place: (0, i, 0)),
                pl.BlockSpec((parts, block, cols), lambda i, place: (0, place[0] * steps + i, 0)),
            ] + [ANY] * len(deps),
            out_specs=pl.BlockSpec((block, width), lambda i, place: (i, 0)),
        ),
        out_shape=jax.ShapeDtypeStruct((rows, width), BF16),
        cost_estimate=pl.CostEstimate(flops=rows * width * 600, bytes_accessed=rows * width * 12, transcendentals=0),
        name="sum_rows",
    )(place, received, hidden, *deps)


def store_kernel(*refs):
    refs[-1][...] = refs[0][...]


def store_rows(y, y_part, first_row, total_rows, deps):
    rows, width = y_part.shape
    block = 128
    return pl.pallas_call(
        store_kernel,
        grid=(rows // block,),
        in_specs=[pl.BlockSpec((block, width), lambda i: (i, 0))] + [ANY] * (len(deps) + (y is not None)),
        out_specs=pl.BlockSpec((block, width), lambda i: (first_row // block + i, 0)),
        out_shape=jax.ShapeDtypeStruct((total_rows, width), BF16),
        input_output_aliases={} if y is None else {1: 0},
        cost_estimate=pl.CostEstimate(flops=rows * width * 300, bytes_accessed=rows * width * 4, transcendentals=0),
        name="store_rows",
    )(*([y_part] if y is None else [y_part, y]), *deps)


def solution(mesh):
    tp_size = mesh.shape["tp"]
    dp_size = mesh.shape["dp"]

    def layer_shard(x, seq_lens, w_query, w_key, w_value, w_out, w_gate, w_up, w_down, attn_gain, mlp_gain, k_cache, v_cache):
        batch_size, seq_len, width = x.shape
        kv_local, head_dim = k_cache.shape[2:]
        q_width = w_query.shape[1]
        tp_index = lax.axis_index("tp")
        dp_index = lax.axis_index("dp")
        place = jnp.stack([tp_index, dp_index]).astype(jnp.int32)
        part_cols = width // tp_size
        total_rows = batch_size * seq_len
        x_rows = x.reshape(total_rows, width)
        chunks = len(CHUNKS)
        first = [sum(CHUNKS[:c]) for c in range(chunks)]

        half = q_width // dp_size
        swaps = [[(i, i ^ hop) for i in range(tp_size)] for hop in range(tp_size)]
        dp_ring = [(i, (i + 1) % dp_size) for i in range(dp_size)]
        mine = []
        other = []
        for hop in range(2, tp_size):
            block = lax.dynamic_slice(w_out, (dp_index * half, (tp_index ^ hop) * part_cols), (half, part_cols))
            mine.append(lax.ppermute(block, "tp", swaps[hop]))
            other.append(lax.ppermute(mine[-1], "dp", dp_ring))
        block = lax.dynamic_slice_in_dim(w_out, (tp_index ^ 1) * part_cols, part_cols, axis=1)
        near = lax.ppermute(block, "tp", swaps[1])

        w_kv = jnp.concatenate([w_key, w_value], axis=1)
        cos_tab, sin_tab = rope_tables(seq_len, head_dim)
        gain = attn_gain.astype(F32).reshape(1, width)
        mlp_gain32 = mlp_gain.astype(F32).reshape(1, width)

        heads = []
        new_keys = []
        new_values = []
        deps = []
        for c in range(chunks):
            rows = CHUNKS[c] * seq_len
            if c == 2:
                deps = deps + [mine[0]]
            qkv = qkv_proj(x_rows, gain, w_query, w_kv, first[c] * seq_len, rows, deps)
            out, keys, values = attention(seq_lens, qkv, cos_tab, sin_tab, first[c], CHUNKS[c], seq_len, head_dim, kv_local, mine[1:] if c == 2 else [])
            deps = [keys]
            heads.append(lax.all_gather(out, "tp", axis=0))
            new_keys.append(keys)
            new_values.append(values)

        hidden = {}
        received = {}
        gathered = {}
        y = None

        def project(c, deps):
            local, token = out_proj(place, heads[c], x_rows, w_out, near, [mine[0], other[0], mine[1], other[1]], first[c] * seq_len, deps)
            hidden[c] = lax.all_gather(local, "tp", axis=0)
            return [token]

        def finish(c, deps):
            y_rows = sum_rows(place, received[c], hidden[c], deps)
            gathered[c] = lax.all_gather(y_rows, "tp", axis=0, tiled=True)
            return [y_rows]

        def store(c, y, deps):
            return store_rows(y, gathered[c], first[c] * seq_len, total_rows, deps)

        deps = project(0, deps)
        deps = project(1, deps)
        for c in range(chunks):
            rows = CHUNKS[c] * seq_len
            gated = gated_proj(hidden[c], mlp_gain32, w_gate, w_up, deps)
            if c == 1:
                project(2, [gated])
            part = jnp.dot(gated, w_down, preferred_element_type=F32).astype(BF16)
            received[c] = lax.all_to_all(part.reshape(tp_size, rows // tp_size, width), "tp", 0, 0, tiled=True)
            deps = [part]
            if c >= 1:
                deps = finish(c - 1, deps)
            if c >= 3:
                y = store(c - 3, y, deps)
                deps = [y]
            if c >= 1 and c + 2 < chunks:
                deps = project(c + 2, deps)

        def cache(old, new):
            new = jnp.concatenate(new, axis=0).reshape(batch_size, seq_len, kv_local, head_dim)
            return jnp.concatenate([new, old[:, seq_len:]], axis=1)

        caches = [cache(k_cache, new_keys), cache(v_cache, new_values)]
        y = store(chunks - 3, y, [])
        finish(chunks - 1, [y] + caches)
        y = store(chunks - 2, y, [])
        y = store(chunks - 1, y, [])

        return y.reshape(x.shape), caches[0], caches[1]

    cache_spec = P("dp", None, "tp", None)
    return jax.shard_map(layer_shard, mesh=mesh, in_specs=(P("dp", None, None), P("dp"), P(None, "tp"), P(None, "tp"), P(None, "tp"), P("tp", None), P(None, "tp"), P(None, "tp"), P("tp", None), P(), P(), cache_spec, cache_spec), out_specs=(P("dp", None, None), cache_spec, cache_spec), check_vma=False)
```
